256 devices in a mesh: vtx: 64 (over z, y_lo, x), src: 4 (over y_hi, core).
Axes of the slice: x: 4, y: 4 (y_hi: 2, y_lo: 2; y = y_hi * 2 + y_lo), z: 8, core: 2. Of those that a mesh axis runs over, the one named last changes fastest.
Arguments:
- heat: float32 [64, 512, 8192], P(None, ('vtx', 'src')), may hold values from -12 to 12
- cotan: float32 [4, 512, 8192], P(None, 'vtx'), may hold values from 0.2 to 2
- source_index: int32 [64], replicated, may hold values from 0 to 4194303
Outputs:
- normalised: float32 [64, 512, 8192], P('src', 'vtx')
- col_norm: float32 [64], P('src')
The draws below stay inside these ranges and needn't reach their ends.
Inputs may be any that keep to these rules, and one draw needn't show every extreme that they name: `source_index`: row-major vertex indices, sources may share a vertex.
All inputs are finite; a program needn't handle non-finite values.
Results may differ from the reference program's by a relative error of at most 0.0003.
Values sent between devices are 32-bit elements; how exact they have to be, the bound alone decides.
A program may use at most 64 MiB of HBM per device.

```python
import math
import jax
import jax.numpy as jnp
from jax import lax

SOURCES = 64
GX = 8192
GY = 512


def draw_heat(key, part):
    rows = jnp.arange(GY, dtype=jnp.float32) / max(GY - 1, 1)
    base_key = jax.random.fold_in(key, 11)
    factor_key = jax.random.fold_in(key, 23)
    row_factor = jax.random.uniform(factor_key, (SOURCES, GY), jnp.float32, 0.3, 1.0)
    base = jnp.clip(jax.random.normal(base_key, (SOURCES, GY, GX), jnp.float32), -4.0, 4.0)
    scale = 1.0 + 2.0 * rows
    return base * (scale[None, :] * row_factor)[:, :, None]


def plant(entries, stream_key, smallest, top_value):
    longest = entries.shape.index(max(entries.shape))
    spots = []
    for shift in (0, 1):
        where = [jax.random.randint(jax.random.fold_in(stream_key, axis), (), 0, length) for axis, length in enumerate(entries.shape)]
        where[longest] = (where[longest] + shift) % entries.shape[longest]
        spots.append(tuple(where))
    return entries.at[spots[0]].set(smallest).at[spots[1]].set(top_value)


def shard_levels(rng, shape, cuts, least, largest):
    loudness, own = 1.0, jax.random.fold_in(rng, 6)
    for axis_at, blocks in cuts:
        heights = jnp.exp(jax.random.uniform(jax.random.fold_in(own, axis_at), (blocks,), jnp.float32, least / len(cuts), largest / len(cuts)))
        loudness = loudness * jnp.repeat(heights, shape[axis_at] // blocks).reshape([-1 if axis == axis_at else 1 for axis in range(len(shape))])
    return loudness


def setup_inputs(seed: int = 0) -> dict:
    streams_of = jax.random.split(jax.random.key(seed), 4)
    return {
        "heat": draw_heat(jax.random.fold_in(streams_of[3], 71), 0),
        "cotan": jnp.clip(jnp.exp(math.log(2.0) - 2.3025851 * jax.random.uniform(streams_of[1], (4, GY, GX), jnp.float32) ** shard_levels(streams_of[1], (4, GY, GX), ((1, 64),), -0.2, 0.2)), 0.2, 2.0),
        "source_index": plant(jax.random.randint(streams_of[2], (SOURCES,), 0, GY * GX), jax.random.fold_in(streams_of[2], 1), 0, (GY * GX) - 1).astype(jnp.int32),
    }


def from_right(values):
    return jnp.concatenate([values[..., 1:], jnp.zeros_like(values[..., :1])], axis=-1)

def from_left(values):
    return jnp.concatenate([jnp.zeros_like(values[..., :1]), values[..., :-1]], axis=-1)

def masked_cotan(cotan, row_start, total_rows):
    shape = cotan.shape[1:]
    rows = row_start + lax.broadcasted_iota(jnp.int32, shape, 0)
    cols = lax.broadcasted_iota(jnp.int32, shape, 1)
    inside_col = cols < shape[1] - 1
    inside_row = rows < total_rows - 1
    mass = cotan[0]
    east = jnp.where(inside_col, cotan[1], 0.0)
    north = jnp.where(inside_row, cotan[2], 0.0)
    diag = jnp.where(inside_col & inside_row, cotan[3], 0.0)
    return (mass, east, north, diag)

def stencil_defect(padded, mass, east, north_ext, diag_ext, row_start, sources, amplitude):
    center = padded[:, 1:-1, :]
    above = padded[:, 2:, :]
    below = padded[:, :-2, :]
    north = north_ext[1:]
    south_weight = north_ext[:-1]
    diag = diag_ext[1:]
    southwest_weight = from_left(diag_ext[:-1])
    west_weight = from_left(east)
    result = mass * center + east * (center - from_right(center))
    result = result + west_weight * (center - from_left(center))
    result = result + north * (center - above) + south_weight * (center - below)
    result = result + diag * (center - from_right(above)) + southwest_weight * (center - from_left(below))
    count_rows, width = (center.shape[1], center.shape[2])
    row_ids = row_start + lax.broadcasted_iota(jnp.int32, (count_rows, width), 0)
    col_ids = lax.broadcasted_iota(jnp.int32, (count_rows, width), 1)
    flat = row_ids * width + col_ids
    delta = (flat[None, :, :] == sources.astype(jnp.int32)[:, None, None]).astype(jnp.float32)
    return result - amplitude * delta

def reference(heat, cotan, source_index):
    total_rows, width = (heat.shape[1], heat.shape[2])
    amplitude = math.sqrt(total_rows * width) / 8.0
    mass, east, north, diag = masked_cotan(cotan, 0, total_rows)
    north_ext = jnp.concatenate([jnp.zeros((1, width), jnp.float32), north], axis=0)
    diag_ext = jnp.concatenate([jnp.zeros((1, width), jnp.float32), diag], axis=0)

    def single(inputs):
        field, source = inputs
        padded = jnp.pad(field[None], ((0, 0), (1, 1), (0, 0)))
        result = stencil_defect(padded, mass, east, north_ext, diag_ext, 0, source[None], amplitude)[0]
        return (result, jnp.sum(result * result))
    defect, squares = lax.map(single, (heat, source_index))
    norms = jnp.sqrt(squares / (total_rows * width) + 1e-06)
    return (defect / norms[:, None, None], norms)
```

```python
import functools
import math

import jax
import jax.numpy as jnp
from jax import lax
from jax.experimental import pallas as pl
from jax.experimental.pallas import tpu as pltpu
from jax.sharding import PartitionSpec as P

MESH = pl.DeviceIdType.MESH
RING = 4
PLANE = 8
GROUP = 2
LANES = 128
F32 = jnp.float32
ABOVE, BELOW = 8, 15


def at(v, k):
    return {"vtx": v, "src": k}


def remote(src, dst, send, recv, target):
    return pltpu.make_async_remote_copy(
        src_ref=src,
        dst_ref=dst,
        send_sem=send,
        recv_sem=recv,
        device_id=target,
        device_id_type=MESH,
    )


def signal(sem, target):
    pl.semaphore_signal(sem, inc=1, device_id=target, device_id_type=MESH)


def each(count, body):
    lax.fori_loop(0, count, lambda i, _: (body(i), 0)[1], 0)


def shifted_weights(cot, lower, weights, v, total_rows, width):
    tiles = width // LANES
    lane = lax.broadcasted_iota(jnp.int32, (8, LANES), 1)
    sub = lax.broadcasted_iota(jnp.int32, (8, LANES), 0)
    in_row = sub + 8 * v < total_rows - 1
    has_lower = jnp.full((8, LANES), v, jnp.int32) > 0

    def tile(j):
        cols = pl.ds(pl.multiple_of(j * LANES, LANES), LANES)
        in_col = lane + j * LANES < width - 1
        east = jnp.where(in_col, cot[1, :, cols], 0.0)
        north = jnp.where(in_row, cot[2, :, cols], 0.0)
        diag = jnp.where(in_col & in_row, cot[3, :, cols], 0.0)
        low_n = jnp.where(has_lower, lower[0, :, cols], 0.0)
        low_d = jnp.where(has_lower & in_col, lower[1, :, cols], 0.0)
        south = jnp.where(sub == 0, low_n, pltpu.roll(north, 1, 0))
        diag_s = jnp.where(sub == 0, low_d, pltpu.roll(diag, 1, 0))
        return cols, east, north, diag, south, diag_s

    def body(j):
        cols, east, north, diag, south, diag_s = tile(j)
        _, east_l, _, diag_l, _, diag_sl = tile(lax.rem(j + tiles - 1, tiles))

        def right(here, left):
            return jnp.where(lane == 0, pltpu.roll(left, 1, 1), pltpu.roll(here, 1, 1))

        west = right(east, east_l)
        diag_w = right(diag, diag_l)
        southwest = right(diag_s, diag_sl)
        weights[0, :, cols] = (
            cot[0, :, cols] + east + west + north + south + diag + southwest
        )
        weights[1, :, cols] = north
        weights[2, :, cols] = south
        weights[3, :, cols] = east
        weights[4, :, cols] = west
        weights[5, :, cols] = diag_w
        weights[6, :, cols] = diag_s

    each(tiles, body)


def field_defect(field, weights, out, s, where, amplitude, width):
    lane = lax.broadcasted_iota(jnp.int32, (8, LANES), 1)
    sub = lax.broadcasted_iota(jnp.int32, (8, LANES), 0)
    flat = sub * width + lane
    step = 8

    def block(b, carry):
        partial, east_at, west_at, acc, rel = carry
        for i in range(step):
            j = b * step + i
            cols = pl.ds(pl.multiple_of(j * LANES, LANES), LANES)
            h = field[s, 0:8, cols]
            halo = field[s, 8:16, cols]
            above = pltpu.roll(jnp.where(sub == 0, halo, h), 7, 0)
            below = pltpu.roll(jnp.where(sub == 7, halo, h), 1, 0)
            to_left = weights[4, :, cols] * h + weights[5, :, cols] * above
            to_right = weights[3, :, cols] * h + weights[6, :, cols] * below
            to_left = pltpu.roll(to_left, LANES - 1, 1)
            to_right = pltpu.roll(to_right, 1, 1)
            done = partial - jnp.where(lane == LANES - 1, to_left, east_at)
            before = pl.ds(
                pl.multiple_of(jnp.maximum(j - 1, 0) * LANES, LANES), LANES
            )
            out[s, :, before] = done
            if i == 0:
                acc = jnp.where(jnp.full((8, LANES), b) > 0, acc + done * done, acc)
            else:
                acc = acc + done * done
            partial = (
                weights[0, :, cols] * h
                - weights[1, :, cols] * above
                - weights[2, :, cols] * below
                - jnp.where(lane == 0, west_at, to_right)
                - jnp.where(flat == rel, amplitude, 0.0)
            )
            east_at, west_at = to_left, to_right
            rel = rel - LANES
        return partial, east_at, west_at, acc, rel

    zero = jnp.zeros((8, LANES), F32)
    rel = jnp.full((8, LANES), where, jnp.int32)
    partial, east_at, _, acc, _ = lax.fori_loop(
        0, width // LANES // step, block, (zero, zero, zero, zero, rel)
    )
    done = partial - jnp.where(lane == LANES - 1, 0.0, east_at)
    out[s, :, width - LANES :] = done
    return acc + done * done


def kernel(
    peers,
    amplitude,
    heat,
    cot_hbm,
    cot,
    sources,
    out,
    norms,
    field,
    lower,
    weights,
    relay,
    row,
    rows,
    own_sem,
    low_send,
    low_recv,
    send,
    recv,
    halo_send,
    halo_recv,
    edge_send,
    relay_send,
    relay_recv,
    sum_send,
    sum_recv,
):
    v, k = lax.axis_index("vtx"), lax.axis_index("src")
    x = lax.rem(v, RING)
    width = field.shape[2]
    per = field.shape[0]
    chunks = per // GROUP
    up, down = lax.rem(v + 1, peers), lax.rem(v + peers - 1, peers)
    line = v - x
    plane = v - lax.rem(v, PLANE)
    top, bottom = k == 3, k == 0
    last, first = x == RING - 1, x == 0

    def in_plane(i):
        inside = lax.rem(v, PLANE)
        return (
            plane
            + lax.rem(inside // RING + i // RING, PLANE // RING) * RING
            + lax.rem(inside + i, RING)
        )

    def in_depth(i):
        return lax.rem(v + PLANE * i, peers)

    depth = peers // PLANE
    barrier = pltpu.get_barrier_semaphore()
    for q in (1, 2, 3):
        signal(barrier, at(v, k ^ q))
    for q in (0, 1):
        signal(barrier, at(up, k ^ q))
        signal(barrier, at(down, k ^ q))
    for i in range(1, PLANE):
        signal(barrier, at(in_plane(i), k))
    for i in range(1, depth):
        signal(barrier, at(in_depth(i), k))
    signal(barrier, at(lax.rem(line + peers - 1, peers), 3))
    signal(barrier, at(lax.rem(line + RING, peers), 0))
    known = 7 + (PLANE - 1) + (depth - 1)
    wraps = (top & last) | (bottom & first)

    @pl.when(wraps)
    def _():
        pl.semaphore_wait(barrier, known + 4 * RING)

    @pl.when(jnp.logical_not(wraps))
    def _():
        pl.semaphore_wait(barrier, known)

    own = pltpu.make_async_copy(
        heat.at[pl.ds(per * k, per)],
        field.at[:, pl.ds(pl.multiple_of(2 * k, 2), 2)],
        own_sem,
    )
    own.start()
    low = remote(
        cot_hbm.at[pl.ds(2, 2), 7], lower.at[:, 0], low_send, low_recv, at(up, k)
    )
    low.start()

    def some(c):
        return pl.ds(c * GROUP, GROUP)

    def edge_copies(c, act):
        for m in range(4):
            data = heat.at[pl.ds(per * m + c * GROUP, GROUP)]
            via = lax.rem(c, RING)
            slot = c // RING

            @pl.when(top & last & (via == 0))
            def _():
                act(
                    remote(
                        data.at[:, 1],
                        field.at[some(c), BELOW],
                        edge_send.at[c, m],
                        halo_recv.at[c, 0],
                        at(up, m),
                    )
                )

            @pl.when(top & last & (via != 0))
            def _():
                act(
                    remote(
                        data.at[:, 1],
                        relay.at[0, slot],
                        edge_send.at[c, m],
                        relay_recv.at[0, slot],
                        at(up + via, m),
                    )
                )

            @pl.when(bottom & first & (via == RING - 1))
            def _():
                act(
                    remote(
                        data.at[:, 0],
                        field.at[some(c), ABOVE],
                        edge_send.at[c, m],
                        halo_recv.at[c, 1],
                        at(down, m),
                    )
                )

            @pl.when(bottom & first & (via != RING - 1))
            def _():
                act(
                    remote(
                        data.at[:, 0],
                        relay.at[1, slot],
                        edge_send.at[c, m],
                        relay_recv.at[1, slot],
                        at(down - (RING - 1) + via, m),
                    )
                )

            if m >= 2:

                @pl.when(top & jnp.logical_not(last))
                def _():
                    act(
                        remote(
                            data.at[:, 1],
                            field.at[some(c), BELOW],
                            edge_send.at[c, m],
                            halo_recv.at[c, 0],
                            at(up, m),
                        )
                    )
            else:

                @pl.when(bottom & jnp.logical_not(first))
                def _():
                    act(
                        remote(
                            data.at[:, 0],
                            field.at[some(c), ABOVE],
                            edge_send.at[c, m],
                            halo_recv.at[c, 1],
                            at(down, m),
                        )
                    )

    start = lambda d: d.start()
    wait_send = lambda d: d.wait_send()
    wait_recv = lambda d: d.wait_recv()

    edge_row = jnp.where(top, 1, 0)

    def exchange(c, i, q, phase):
        to = k ^ q
        r = edge_row if phase == 0 else 1 - edge_row
        return remote(
            heat.at[pl.ds(per * to + c * GROUP, GROUP), r],
            field.at[some(c), 2 * k + r],
            send.at[c, i, phase],
            recv.at[c, i, phase],
            at(v, to),
        )

    def begin(c):
        exchange(c, 0, 2, 0).start()
        exchange(c, 1, 3, 0).start()
        edge_copies(c, start)

    each(chunks, begin)

    def begin_rest(c):
        exchange(c, 2, 1, 0).start()
        exchange(c, 2, 1, 1).start()
        exchange(c, 0, 2, 1).start()
        exchange(c, 1, 3, 1).start()

    each(chunks, begin_rest)

    low.wait_recv()
    shifted_weights(cot, lower, weights, v, peers * 8, width)

    came = jnp.where((k == 0) | (k == 3), 1, 0)
    inner_up = (k < 2) & jnp.logical_not(last)
    inner_down = (k >= 2) & jnp.logical_not(first)

    def forward(c, act):
        @pl.when(inner_up)
        def _():
            act(
                remote(
                    field.at[some(c), 7],
                    field.at[some(c), BELOW],
                    halo_send.at[c],
                    halo_recv.at[c, 0],
                    at(up, k),
                )
            )

        @pl.when(inner_down)
        def _():
            act(
                remote(
                    field.at[some(c), 0],
                    field.at[some(c), ABOVE],
                    halo_send.at[c],
                    halo_recv.at[c, 1],
                    at(down, k),
                )
            )

    def relayed(slot, act):
        c = x + RING * slot

        @pl.when(jnp.logical_not(first))
        def _():
            act(
                remote(
                    relay.at[0, slot],
                    field.at[some(c), BELOW],
                    relay_send.at[0, slot],
                    halo_recv.at[c, 0],
                    at(line, k),
                ),
                0,
                slot,
            )

        @pl.when(jnp.logical_not(last))
        def _():
            act(
                remote(
                    relay.at[1, slot],
                    field.at[some(c), ABOVE],
                    relay_send.at[1, slot],
                    halo_recv.at[c, 1],
                    at(line + RING - 1, k),
                ),
                1,
                slot,
            )

    def relay_on(copy, side, slot):
        arrived(relay.at[side, slot], relay_recv.at[side, slot])
        copy.start()

    def arrived(ref, sem):
        pltpu.make_async_copy(ref, ref, sem).wait()

    def pass_on(c):
        arrived(field.at[some(c), 0], recv.at[c, came, 0])
        forward(c, start)

    for slot in range(chunks // RING):
        for c in range(slot * RING, (slot + 1) * RING):
            pass_on(c)
        relayed(slot, relay_on)

    own.wait()
    lane = lax.broadcasted_iota(jnp.int32, (1, LANES), 1)
    base = v * (8 * width)

    def chunk(c, sums):
        arrived(field.at[some(c), 0], recv.at[c, 1 - came, 0])
        arrived(field.at[some(c), 0], recv.at[c, 2, 0])
        for i in range(3):
            arrived(field.at[some(c), 0], recv.at[c, i, 1])
        for i in range(2):
            arrived(field.at[some(c), 0], halo_recv.at[c, i])

        def one(g, sums):
            s = c * GROUP + g
            acc = field_defect(
                field, weights, out, s, sources[per * k + s] - base, amplitude, width
            )
            total = jnp.sum(acc, axis=(0, 1), keepdims=True)
            return sums + jnp.where(lane == s, total, 0.0)

        return lax.fori_loop(0, GROUP, one, sums)

    sums = lax.fori_loop(0, chunks, chunk, jnp.zeros((1, LANES), F32))

    def exchanged(which, value, count, place, back):
        row[which] = value
        copies = []
        for i in range(1, count):
            copies.append(
                remote(
                    row.at[which],
                    rows.at[which, back(i)],
                    sum_send.at[which, i],
                    sum_recv.at[which, back(i)],
                    at(place(i), k),
                )
            )
            copies[-1].start()
        for i in range(1, count):
            arrived(row.at[which], sum_recv.at[which, i])
            value = value + rows[which, i]
        return value, copies

    sums, sent = exchanged(
        0,
        sums,
        PLANE,
        in_plane,
        lambda i: (i // RING) * RING + (RING - i % RING) % RING,
    )
    sums, more = exchanged(1, sums, depth, in_depth, lambda i: depth - i)
    norms[...] = jnp.sqrt(sums / (peers * 8 * width) + 1e-06)

    for copy in sent + more:
        copy.wait_send()
    low.wait_send()

    def left(c):
        for phase in range(2):
            exchange(c, 0, 2, phase).wait_send()
            exchange(c, 1, 3, phase).wait_send()
            exchange(c, 2, 1, phase).wait_send()
        edge_copies(c, wait_send)
        forward(c, wait_send)

    each(chunks, left)
    for slot in range(chunks // RING):
        relayed(slot, lambda copy, side, slot: copy.wait_send())


def on_device(heat, cotan, source_index):
    peers = lax.axis_size("vtx")
    rows_dev, width = cotan.shape[1:]
    per = heat.shape[0] // lax.axis_size("src")
    chunks = per // GROUP
    amplitude = math.sqrt(rows_dev * peers * width) / 8.0
    dma, vmem = pltpu.SemaphoreType.DMA, pltpu.VMEM
    anywhere = pl.BlockSpec(memory_space=pl.ANY)
    held = pl.BlockSpec(memory_space=pltpu.VMEM)
    defect, norms = pl.pallas_call(
        functools.partial(kernel, peers, amplitude),
        name="defect",
        out_shape=(
            jax.ShapeDtypeStruct((per, rows_dev, width), F32),
            jax.ShapeDtypeStruct((1, LANES), F32),
        ),
        in_specs=[
            anywhere,
            anywhere,
            held,
            pl.BlockSpec(memory_space=pltpu.SMEM),
        ],
        out_specs=(held, held),
        scratch_shapes=[
            vmem((per, 2 * rows_dev, width), F32),
            vmem((2, 8, width), F32),
            vmem((7, rows_dev, width), F32),
            vmem((2, chunks // RING, GROUP, width), F32),
            vmem((2, 1, LANES), F32),
            vmem((2, PLANE, 1, LANES), F32),
            dma,
            dma,
            dma,
            dma((chunks, 3, 2)),
            dma((chunks, 3, 2)),
            dma((chunks,)),
            dma((chunks, 2)),
            dma((chunks, 4)),
            dma((2, chunks // RING)),
            dma((2, chunks // RING)),
            dma((2, PLANE)),
            dma((2, PLANE)),
        ],
        compiler_params=pltpu.CompilerParams(
            collective_id=0, has_side_effects=True, vmem_limit_bytes=40 << 20
        ),
        cost_estimate=pl.CostEstimate(
            flops=200_000_000, bytes_accessed=16_000_000, transcendentals=0
        ),
    )(heat, cotan, cotan, source_index)
    norms = norms[0, :per]
    return (defect / norms[:, None, None], norms)


def solution(mesh):
    return jax.shard_map(
        on_device,
        mesh=mesh,
        in_specs=(P(None, ("vtx", "src"), None), P(None, "vtx", None), P()),
        out_specs=(P("src", "vtx", None), P("src")),
        check_vma=False,
    )
```

```python
import functools
import math

import jax
import jax.numpy as jnp
from jax import lax
from jax.experimental import pallas as pl
from jax.experimental.pallas import tpu as pltpu
from jax.sharding import PartitionSpec as P

MESH = pl.DeviceIdType.MESH
RING = 4
PLANE = 8
GROUP = 4
PIECE = 2
LATE = 1
LANES = 128
F32 = jnp.float32
ABOVE, BELOW = 8, 15


def at(v, k):
    return {"vtx": v, "src": k}


def remote(src, dst, send, recv, target):
    return pltpu.make_async_remote_copy(
        src_ref=src,
        dst_ref=dst,
        send_sem=send,
        recv_sem=recv,
        device_id=target,
        device_id_type=MESH,
    )


def signal(sem, target):
    pl.semaphore_signal(sem, inc=1, device_id=target, device_id_type=MESH)


def each(count, body):
    lax.fori_loop(0, count, lambda i, _: (body(i), 0)[1], 0)


def shifted_weights(cot, lower, weights, v, total_rows, width):
    tiles = width // LANES
    step = 8
    lane = lax.broadcasted_iota(jnp.int32, (8, LANES), 1)
    sub = lax.broadcasted_iota(jnp.int32, (8, LANES), 0)
    in_row = sub + 8 * v < total_rows - 1
    has_lower = jnp.full((8, LANES), v, jnp.int32) > 0
    zero = jnp.zeros((8, LANES), F32)

    def block(b, carry):
        for i in range(step):
            j = b * step + i
            cols = pl.ds(pl.multiple_of(j * LANES, LANES), LANES)
            in_col = lane + j * LANES < width - 1
            east = jnp.where(in_col, cot[1, :, cols], 0.0)
            north = jnp.where(in_row, cot[2, :, cols], 0.0)
            diag = jnp.where(in_col & in_row, cot[3, :, cols], 0.0)
            low_n = jnp.where(has_lower, lower[0, :, cols], 0.0)
            low_d = jnp.where(has_lower & in_col, lower[1, :, cols], 0.0)
            south = jnp.where(sub == 0, low_n, pltpu.roll(north, 1, 0))
            diag_s = jnp.where(sub == 0, low_d, pltpu.roll(diag, 1, 0))
            turned = tuple(pltpu.roll(w, 1, 1) for w in (east, diag, diag_s))
            west, diag_w, southwest = (
                jnp.where(lane == 0, left, here) for left, here in zip(carry, turned)
            )
            weights[0, :, cols] = (
                cot[0, :, cols] + east + west + north + south + diag + southwest
            )
            weights[1, :, cols] = north
            weights[2, :, cols] = south
            weights[3, :, cols] = east
            weights[4, :, cols] = west
            weights[5, :, cols] = diag_w
            weights[6, :, cols] = diag_s
            carry = turned
        return carry

    lax.fori_loop(0, tiles // step, block, (zero, zero, zero))


def field_defect(field, weights, out, s, where, amplitude, width):
    lane = lax.broadcasted_iota(jnp.int32, (8, LANES), 1)
    sub = lax.broadcasted_iota(jnp.int32, (8, LANES), 0)
    spot = where - (sub * width + lane)
    zero = jnp.zeros((8, LANES), F32)
    sums = [zero, zero]
    partial, east_at, west_at = None, None, zero

    def finish(j, to_left):
        done = partial - jnp.where(lane == LANES - 1, to_left, east_at)
        out[s, :, j * LANES : (j + 1) * LANES] = done
        sums[j % 2] = sums[j % 2] + done * done

    tiles = width // LANES
    for j in range(tiles):
        cols = slice(j * LANES, (j + 1) * LANES)
        h = field[s, 0:8, cols]
        halo = field[s, 8:16, cols]
        above = pltpu.roll(jnp.where(sub == 0, halo, h), 7, 0)
        below = pltpu.roll(jnp.where(sub == 7, halo, h), 1, 0)
        to_left = weights[4, :, cols] * h + weights[5, :, cols] * above
        to_right = weights[3, :, cols] * h + weights[6, :, cols] * below
        to_left = pltpu.roll(to_left, LANES - 1, 1)
        to_right = pltpu.roll(to_right, 1, 1)
        if j > 0:
            finish(j - 1, to_left)
        partial = (
            weights[0, :, cols] * h
            - weights[1, :, cols] * above
            - weights[2, :, cols] * below
            - jnp.where(lane == 0, west_at, to_right)
            - jnp.where(spot == j * LANES, amplitude, 0.0)
        )
        east_at, west_at = to_left, to_right
    finish(tiles - 1, zero)
    return sums[0] + sums[1]


def kernel(
    peers,
    amplitude,
    heat,
    cot_hbm,
    sources_hbm,
    out,
    norms,
    cot,
    sources,
    field,
    lower,
    weights,
    relay,
    row,
    rows,
    spare,
    known,
    own_sem,
    cot_sem,
    src_sem,
    low_send,
    low_recv,
    part_send,
    part_recv,
    hand_send,
    hand_recv,
    send,
    first_recv,
    near_recv,
    second_recv,
    edge_send,
    halo_send,
    halo_recv,
    relay_send,
    relay_recv,
    sum_send,
    sum_recv,
):
    v, k = lax.axis_index("vtx"), lax.axis_index("src")
    x = lax.rem(v, RING)
    per, _, width = field.shape
    groups, pieces = per // GROUP, per // PIECE
    up, down = lax.rem(v + 1, peers), lax.rem(v + peers - 1, peers)
    line = v - x
    top, bottom = k == 3, k == 0
    last, first = x == RING - 1, x == 0

    around = [line + lax.rem(x + i, RING) for i in range(1, RING)]
    across = v + RING - 2 * RING * lax.rem(v // RING, 2)
    depth = [lax.rem(v + PLANE, peers), lax.rem(v + peers - PLANE, peers)]
    shared = [at(v, k ^ q) for q in (2, 3, 1)]
    around, across, depth = (
        [at(i, k) for i in around],
        [at(across, k)],
        [at(i, k) for i in depth],
    )

    cot_copy = pltpu.make_async_copy(cot_hbm, cot, cot_sem)
    cot_copy.start()
    src_copy = pltpu.make_async_copy(sources_hbm, sources, src_sem)
    src_copy.start()
    own = pltpu.make_async_copy(
        heat.at[pl.ds(per * k, per)],
        field.at[:, pl.ds(pl.multiple_of(2 * k, 2), 2)],
        own_sem,
    )
    own.start()
    barrier = pltpu.get_barrier_semaphore()
    near = shared + around + across + depth
    for target in near:
        signal(barrier, target)
    pl.semaphore_wait(barrier, len(near))

    def some(start, count):
        return pl.ds(start, count)

    def arrived(ref, sem):
        pltpu.make_async_copy(ref, ref, sem).wait()

    edge_row = jnp.where(top, 1, 0)

    def exchange(i, q, r, start, count, sem):
        return remote(
            heat.at[pl.ds(per * (k ^ q) + start, count), r],
            field.at[some(start, count), 2 * k + r],
            send,
            sem,
            at(v, k ^ q),
        )

    def begin(g):
        for i, q in enumerate((2, 3)):
            exchange(i, q, edge_row, g * GROUP, GROUP, first_recv.at[g, i]).start()

    begin(0)

    above_side, below_side = last & (k >= 2), first & (k < 2)
    holds = top | bottom
    own_row = jnp.where(top, 1, 0)
    block_row = jnp.where(k >= 2, 7, 0)
    split = (above_side | below_side) & holds
    helps = (above_side | below_side) & jnp.logical_not(holds)
    handed = remote(
        heat.at[pl.ds(per * (k ^ 3), per), own_row],
        spare,
        hand_send,
        hand_recv,
        at(v, k ^ 1),
    )

    @pl.when(split)
    def _():
        handed.start()

    def begin_near(g):
        remote(
            heat.at[pl.ds(per * (k ^ 1) + g * GROUP, GROUP)],
            field.at[some(g * GROUP, GROUP), pl.ds(pl.multiple_of(2 * k, 2), 2)],
            send,
            near_recv.at[g],
            at(v, k ^ 1),
        ).start()

    each(groups, begin_near)

    def meet(stage, targets):
        for target in targets:
            signal(known.at[stage], target)
        pl.semaphore_wait(known.at[stage], len(targets))

    meet(0, around)
    meet(1, across)
    meet(2, shared)

    half = width // 2
    cut = pl.ds(pl.multiple_of(lax.rem(k, 2) * half, half), half)
    low = remote(
        cot_hbm.at[pl.ds(2, 2), 7, cut],
        lower.at[:, 0, cut],
        low_send,
        low_recv,
        at(up, k),
    )
    low.start()

    for g in range(groups):
        arrived(field.at[some(g * GROUP, GROUP), 0:2], near_recv.at[g])

    @pl.when(helps)
    def _():
        handed.wait_recv()

    def wrap_copies(c):
        via = lax.rem(c, RING)
        slot = c // RING
        span = some(c * PIECE, PIECE)
        sem = c * PIECE // GROUP

        def send_on(src, m):
            for side, active, end, hop in (
                (0, above_side, 0, up),
                (1, below_side, RING - 1, down - (RING - 1)),
            ):

                @pl.when(active & (via == end))
                def _():
                    remote(
                        src,
                        field.at[span, (BELOW, ABOVE)[side]],
                        edge_send,
                        halo_recv.at[sem, side],
                        at(hop + via, m),
                    ).start()

                @pl.when(active & (via != end))
                def _():
                    remote(
                        src,
                        relay.at[side, slot],
                        edge_send,
                        relay_recv.at[side, slot],
                        at(hop + via, m),
                    ).start()

        @pl.when(split)
        def _():
            for m in (k, k ^ 2):
                send_on(heat.at[pl.ds(per * m + c * PIECE, PIECE), own_row], m)

        @pl.when(helps)
        def _():
            send_on(field.at[span, block_row], k)
            send_on(spare.at[span], k ^ 2)

    each(pieces, wrap_copies)

    def edge_copies(g):
        span = some(g * GROUP, GROUP)
        for i in range(2):

            @pl.when(top & jnp.logical_not(last))
            def _():
                m = 2 + i
                remote(
                    heat.at[pl.ds(per * m + g * GROUP, GROUP), 1],
                    field.at[span, BELOW],
                    edge_send,
                    halo_recv.at[g, 0],
                    at(up, m),
                ).start()

            @pl.when(bottom & jnp.logical_not(first))
            def _():
                remote(
                    heat.at[pl.ds(per * i + g * GROUP, GROUP), 0],
                    field.at[span, ABOVE],
                    edge_send,
                    halo_recv.at[g, 1],
                    at(down, i),
                ).start()

    each(groups, edge_copies)

    lax.fori_loop(1, groups, lambda g, _: (begin(g), 0)[1], 0)

    def begin_second(b):
        for i, q in enumerate((2, 3)):
            exchange(
                i, q, 1 - edge_row, b * LATE, LATE, second_recv.at[b, i]
            ).start()

    each(per // LATE, begin_second)

    arrived(lower.at[:, 0, cut], low_recv)
    part = remote(
        lower.at[:, 0, cut], lower.at[:, 0, cut], part_send, part_recv, at(v, k ^ 1)
    )
    part.start()
    cot_copy.wait()
    src_copy.wait()
    part.wait_recv()
    shifted_weights(cot, lower, weights, v, peers * 8, width)
    meet(3, depth)

    came = jnp.where((k == 0) | (k == 3), 1, 0)
    inner_up = (k < 2) & jnp.logical_not(last)
    inner_down = (k >= 2) & jnp.logical_not(first)

    def forward(g):
        span = some(g * GROUP, GROUP)

        @pl.when(inner_up)
        def _():
            remote(
                field.at[span, 7],
                field.at[span, BELOW],
                halo_send,
                halo_recv.at[g, 0],
                at(up, k),
            ).start()

        @pl.when(inner_down)
        def _():
            remote(
                field.at[span, 0],
                field.at[span, ABOVE],
                halo_send,
                halo_recv.at[g, 1],
                at(down, k),
            ).start()

    def relayed(slot):
        c = x + RING * slot
        span = some(c * PIECE, PIECE)
        sem = c * PIECE // GROUP

        @pl.when(jnp.logical_not(first))
        def _():
            arrived(relay.at[0, slot], relay_recv.at[0, slot])
            remote(
                relay.at[0, slot],
                field.at[span, BELOW],
                relay_send.at[0],
                halo_recv.at[sem, 0],
                at(line, k),
            ).start()

        @pl.when(jnp.logical_not(last))
        def _():
            arrived(relay.at[1, slot], relay_recv.at[1, slot])
            remote(
                relay.at[1, slot],
                field.at[span, ABOVE],
                relay_send.at[1],
                halo_recv.at[sem, 1],
                at(line + RING - 1, k),
            ).start()

    for g in range(groups):
        arrived(field.at[some(g * GROUP, GROUP), 0], first_recv.at[g, came])
        forward(g)
        if g % 2 == 1:
            meet(4 + g // 2, depth)

    own.wait()
    lane = lax.broadcasted_iota(jnp.int32, (1, LANES), 1)
    base = v * (8 * width)

    slots = pieces // RING

    def group(g, sums):
        span = some(g * GROUP, GROUP)

        @pl.when(lax.rem(g, groups // slots) == 0)
        def _():
            relayed(g // (groups // slots))

        arrived(field.at[span, 0], first_recv.at[g, 1 - came])
        for i in range(2):
            arrived(field.at[span, 0], halo_recv.at[g, i])

        def late(b, sums):
            for i in range(2):
                arrived(field.at[some(b * LATE, LATE), 0], second_recv.at[b, i])

            def one(s, sums):
                acc = field_defect(
                    field,
                    weights,
                    out,
                    s,
                    sources[per * k + s] - base,
                    amplitude,
                    width,
                )
                total = jnp.sum(acc, axis=(0, 1), keepdims=True)
                return sums + jnp.where(lane == s, total, 0.0)

            return lax.fori_loop(b * LATE, (b + 1) * LATE, one, sums)

        share = GROUP // LATE
        return lax.fori_loop(g * share, (g + 1) * share, late, sums)

    sums = lax.fori_loop(0, groups, group, jnp.zeros((1, LANES), F32))

    row[...] = sums

    def tell(i):
        remote(row, rows.at[i], sum_send, sum_recv, at(lax.rem(v + i, peers), k)).start()

    lax.fori_loop(1, peers, lambda i, _: (tell(i), 0)[1], 0)

    low.wait_send()
    part.wait_send()
    sizes = (field.at[0 : 3 * per // 4, 0:8], send)
    arrived(*sizes)

    @pl.when(split)
    def _():
        handed.wait_send()

    wraps = above_side | below_side
    inner = (top & jnp.logical_not(last)) | (bottom & jnp.logical_not(first))

    @pl.when(wraps | inner)
    def _():
        arrived(field.at[:, 0:2], edge_send)

    @pl.when(inner_up | inner_down)
    def _():
        arrived(field.at[:, 0:1], halo_send)

    @pl.when(jnp.logical_not(first))
    def _():
        arrived(relay.at[0], relay_send.at[0])

    @pl.when(jnp.logical_not(last))
    def _():
        arrived(relay.at[1], relay_send.at[1])

    arrived(rows.at[1:peers], sum_recv)
    sums = sums + jnp.sum(rows[1:peers], axis=0)
    norms[...] = jnp.sqrt(sums / (peers * 8 * width) + 1e-06)
    arrived(rows.at[1:peers], sum_send)


def scale(defect, norms, out, held, sem):
    per = defect.shape[0]
    lane = lax.broadcasted_iota(jnp.int32, (per, LANES), 1)
    which = lax.broadcasted_iota(jnp.int32, (per, LANES), 0)
    own = jnp.where(lane == which, norms[...], 0.0)
    inverse = 1.0 / jnp.sum(own, axis=1, keepdims=True)
    copies = []
    for s in range(per):
        held[s] = defect[s] * inverse[s : s + 1]
        copies.append(pltpu.make_async_copy(held.at[s], out.at[s], sem.at[s]))
        copies[-1].start()
    for copy in copies:
        copy.wait()


def on_device(heat, cotan, source_index):
    peers = lax.axis_size("vtx")
    rows_dev, width = cotan.shape[1:]
    per = heat.shape[0] // lax.axis_size("src")
    groups, slots = per // GROUP, per // PIECE // RING
    amplitude = math.sqrt(rows_dev * peers * width) / 8.0
    dma, vmem = pltpu.SemaphoreType.DMA, pltpu.VMEM
    anywhere = pl.BlockSpec(memory_space=pl.ANY)
    held = pl.BlockSpec(memory_space=pltpu.VMEM)
    block = jax.ShapeDtypeStruct((per, rows_dev, width), F32)
    defect, norms = pl.pallas_call(
        functools.partial(kernel, peers, amplitude),
        name="defect",
        out_shape=(block, jax.ShapeDtypeStruct((1, LANES), F32)),
        in_specs=[anywhere] * 3,
        out_specs=(held, held),
        scratch_shapes=[
            vmem((4, rows_dev, width), F32),
            pltpu.SMEM(source_index.shape, jnp.int32),
            vmem((per, 2 * rows_dev, width), F32),
            vmem((2, 8, width), F32),
            vmem((7, rows_dev, width), F32),
            vmem((2, slots, PIECE, width), F32),
            vmem((1, LANES), F32),
            vmem((peers, 1, LANES), F32),
            vmem((per, width), F32),
            pltpu.SemaphoreType.REGULAR((6,)),
            dma,
            dma,
            dma,
            dma,
            dma,
            dma,
            dma,
            dma,
            dma,
            dma,
            dma((groups, 2)),
            dma((groups,)),
            dma((per // LATE, 2)),
            dma,
            dma,
            dma((groups, 2)),
            dma((2,)),
            dma((2, slots)),
            dma,
            dma,
        ],
        compiler_params=pltpu.CompilerParams(
            collective_id=0, has_side_effects=True, vmem_limit_bytes=40 << 20
        ),
        cost_estimate=pl.CostEstimate(
            flops=200_000_000, bytes_accessed=16_000_000, transcendentals=0
        ),
    )(
        *(
            pltpu.with_memory_space_constraint(a, pltpu.HBM)
            for a in (heat, cotan, source_index)
        )
    )
    norms, col_norm = lax.optimization_barrier((norms, norms[0, :per]))
    normalised = pl.pallas_call(
        scale,
        name="scale",
        out_shape=block,
        in_specs=[held, held],
        out_specs=anywhere,
        scratch_shapes=[vmem(block.shape, F32), dma((per,))],
        compiler_params=pltpu.CompilerParams(vmem_limit_bytes=16 << 20),
    )(defect, norms)
    return (normalised, col_norm)


def solution(mesh):
    return jax.shard_map(
        on_device,
        mesh=mesh,
        in_specs=(P(None, ("vtx", "src"), None), P(None, "vtx", None), P()),
        out_specs=(P("src", "vtx", None), P("src")),
        check_vma=False,
    )
```

```python
import functools
import math

import jax
import jax.numpy as jnp
from jax import lax
from jax.experimental import pallas as pl
from jax.experimental.pallas import tpu as pltpu
from jax.sharding import PartitionSpec as P

MESH = pl.DeviceIdType.MESH
RING = 4
PLANE = 8
GROUP = 4
PIECE = 2
TELL = 9
LANES = 128
F32 = jnp.float32
ABOVE, BELOW = 8, 15


def at(v, k):
    return {"vtx": v, "src": k}


def remote(src, dst, send, recv, target):
    return pltpu.make_async_remote_copy(
        src_ref=src,
        dst_ref=dst,
        send_sem=send,
        recv_sem=recv,
        device_id=target,
        device_id_type=MESH,
    )


def signal(sem, target):
    pl.semaphore_signal(sem, inc=1, device_id=target, device_id_type=MESH)


def each(count, body):
    lax.fori_loop(0, count, lambda i, _: (body(i), 0)[1], 0)


def shifted_weights(cot, lower, weights, v, total_rows, width):
    tiles = width // LANES
    step = 8
    lane = lax.broadcasted_iota(jnp.int32, (8, LANES), 1)
    sub = lax.broadcasted_iota(jnp.int32, (8, LANES), 0)
    in_row = sub + 8 * v < total_rows - 1
    has_lower = jnp.full((8, LANES), v, jnp.int32) > 0
    zero = jnp.zeros((8, LANES), F32)

    def block(b, carry):
        for i in range(step):
            j = b * step + i
            cols = pl.ds(pl.multiple_of(j * LANES, LANES), LANES)
            in_col = lane + j * LANES < width - 1
            east = jnp.where(in_col, cot[1, :, cols], 0.0)
            north = jnp.where(in_row, cot[2, :, cols], 0.0)
            diag = jnp.where(in_col & in_row, cot[3, :, cols], 0.0)
            low_n = jnp.where(has_lower, lower[0, :, cols], 0.0)
            low_d = jnp.where(has_lower & in_col, lower[1, :, cols], 0.0)
            south = jnp.where(sub == 0, low_n, pltpu.roll(north, 1, 0))
            diag_s = jnp.where(sub == 0, low_d, pltpu.roll(diag, 1, 0))
            turned = tuple(pltpu.roll(w, 1, 1) for w in (east, diag, diag_s))
            west, diag_w, southwest = (
                jnp.where(lane == 0, left, here) for left, here in zip(carry, turned)
            )
            weights[0, :, cols] = (
                cot[0, :, cols] + east + west + north + south + diag + southwest
            )
            weights[1, :, cols] = north
            weights[2, :, cols] = south
            weights[3, :, cols] = east
            weights[4, :, cols] = west
            weights[5, :, cols] = diag_w
            weights[6, :, cols] = diag_s
            carry = turned
        return carry

    lax.fori_loop(0, tiles // step, block, (zero, zero, zero))


def field_defect(field, weights, out, s, where, amplitude, width):
    lane = lax.broadcasted_iota(jnp.int32, (8, LANES), 1)
    sub = lax.broadcasted_iota(jnp.int32, (8, LANES), 0)
    spot = where - (sub * width + lane)
    zero = jnp.zeros((8, LANES), F32)
    sums = [zero, zero]
    partial, east_at, west_at = None, None, zero

    def finish(j, to_left):
        done = partial - jnp.where(lane == LANES - 1, to_left, east_at)
        out[s, :, j * LANES : (j + 1) * LANES] = done
        sums[j % 2] = sums[j % 2] + done * done

    tiles = width // LANES
    for j in range(tiles):
        cols = slice(j * LANES, (j + 1) * LANES)
        h = field[s, 0:8, cols]
        halo = field[s, 8:16, cols]
        above = pltpu.roll(jnp.where(sub == 0, halo, h), 7, 0)
        below = pltpu.roll(jnp.where(sub == 7, halo, h), 1, 0)
        to_left = weights[4, :, cols] * h + weights[5, :, cols] * above
        to_right = weights[3, :, cols] * h + weights[6, :, cols] * below
        to_left = pltpu.roll(to_left, LANES - 1, 1)
        to_right = pltpu.roll(to_right, 1, 1)
        if j > 0:
            finish(j - 1, to_left)
        partial = (
            weights[0, :, cols] * h
            - weights[1, :, cols] * above
            - weights[2, :, cols] * below
            - jnp.where(lane == 0, west_at, to_right)
            - jnp.where(spot == j * LANES, amplitude, 0.0)
        )
        east_at, west_at = to_left, to_right
    finish(tiles - 1, zero)
    return sums[0] + sums[1]


def kernel(
    peers,
    amplitude,
    heat,
    cot_hbm,
    sources_hbm,
    out,
    norms,
    cot,
    sources,
    field,
    lower,
    weights,
    relay,
    row,
    rows,
    spare,
    known,
    own_sem,
    cot_sem,
    src_sem,
    low_send,
    low_recv,
    part_recv,
    hand_recv,
    send,
    first_recv,
    near_recv,
    second_recv,
    edge_send,
    halo_send,
    halo_recv,
    relay_send,
    relay_recv,
    sum_send,
    sum_recv,
):
    v, k = lax.axis_index("vtx"), lax.axis_index("src")
    x = lax.rem(v, RING)
    per, _, width = field.shape
    groups, pieces = per // GROUP, per // PIECE
    tail = per - GROUP
    up, down = lax.rem(v + 1, peers), lax.rem(v + peers - 1, peers)
    line = v - x
    top, bottom = k == 3, k == 0
    last, first = x == RING - 1, x == 0

    around = [line + lax.rem(x + i, RING) for i in range(1, RING)]
    across = v + RING - 2 * RING * lax.rem(v // RING, 2)
    depth = [lax.rem(v + PLANE, peers), lax.rem(v + peers - PLANE, peers)]
    shared = [at(v, k ^ q) for q in (2, 3, 1)]
    around, across, depth = (
        [at(i, k) for i in around],
        [at(across, k)],
        [at(i, k) for i in depth],
    )

    cot_copy = pltpu.make_async_copy(cot_hbm, cot, cot_sem)
    cot_copy.start()
    src_copy = pltpu.make_async_copy(sources_hbm, sources, src_sem)
    src_copy.start()
    own = pltpu.make_async_copy(
        heat.at[pl.ds(per * k, per)],
        field.at[:, pl.ds(pl.multiple_of(2 * k, 2), 2)],
        own_sem,
    )
    own.start()
    barrier = pltpu.get_barrier_semaphore()
    near = shared + around + across + depth
    for target in near:
        signal(barrier, target)
    pl.semaphore_wait(barrier, len(near))

    def some(start, count):
        return pl.ds(start, count)

    def arrived(ref, sem):
        pltpu.make_async_copy(ref, ref, sem).wait()

    edge_row = jnp.where(top, 1, 0)

    def exchange(q, r, start, count, sem):
        return remote(
            heat.at[pl.ds(per * (k ^ q) + start, count), r],
            field.at[some(start, count), 2 * k + r],
            send,
            sem,
            at(v, k ^ q),
        )

    def begin(g):
        for q in (2, 3):
            exchange(q, edge_row, g * GROUP, GROUP, first_recv.at[g]).start()

    begin(0)

    above_side = last & (k >= 2)
    below_side = first & (k < 2)
    holds = top | bottom
    own_row = jnp.where(top, 1, 0)
    block_row = jnp.where(k >= 2, 7, 0)
    split = (above_side | below_side) & holds
    helps = (above_side | below_side) & jnp.logical_not(holds)
    handed = remote(
        heat.at[pl.ds(per * (k ^ 3), per), own_row],
        spare,
        edge_send,
        hand_recv,
        at(v, k ^ 1),
    )

    @pl.when(split)
    def _():
        handed.start()

    def begin_near(g):
        remote(
            heat.at[pl.ds(per * (k ^ 1) + g * GROUP, GROUP)],
            field.at[some(g * GROUP, GROUP), pl.ds(pl.multiple_of(2 * k, 2), 2)],
            send,
            near_recv,
            at(v, k ^ 1),
        ).start()

    each(groups, begin_near)

    def meet(stage, targets):
        for target in targets:
            signal(known.at[stage], target)
        pl.semaphore_wait(known.at[stage], len(targets))

    meet(0, around)
    meet(1, across)
    meet(2, shared)

    half = width // 2
    cut = pl.ds(pl.multiple_of(lax.rem(k, 2) * half, half), half)
    low = remote(
        cot_hbm.at[pl.ds(2, 2), 7, cut],
        lower.at[:, 0, cut],
        low_send,
        low_recv,
        at(up, k),
    )
    low.start()

    arrived(field.at[:, 0:2], near_recv)

    @pl.when(helps)
    def _():
        handed.wait_recv()

    def wrap_copies(c):
        via = lax.rem(c, RING)
        slot = c // RING
        span = some(c * PIECE, PIECE)
        sem = c * PIECE // GROUP

        def send_on(src, m):
            for side, active, end, hop in (
                (0, above_side, 0, up),
                (1, below_side, RING - 1, down - (RING - 1)),
            ):

                @pl.when(active & (via == end))
                def _():
                    remote(
                        src,
                        field.at[span, (BELOW, ABOVE)[side]],
                        edge_send,
                        halo_recv.at[sem],
                        at(hop + via, m),
                    ).start()

                @pl.when(active & (via != end))
                def _():
                    remote(
                        src,
                        relay.at[side, slot],
                        edge_send,
                        relay_recv.at[side, slot],
                        at(hop + via, m),
                    ).start()

        @pl.when(split)
        def _():
            for m in (k, k ^ 2):
                send_on(heat.at[pl.ds(per * m + c * PIECE, PIECE), own_row], m)

        @pl.when(helps)
        def _():
            send_on(field.at[span, block_row], k)
            send_on(spare.at[span], k ^ 2)

    each(pieces, wrap_copies)

    def edge_copies(g):
        span = some(g * GROUP, GROUP)
        for i in range(2):

            @pl.when(top & jnp.logical_not(last))
            def _():
                m = 2 + i
                remote(
                    heat.at[pl.ds(per * m + g * GROUP, GROUP), 1],
                    field.at[span, BELOW],
                    edge_send,
                    halo_recv.at[g],
                    at(up, m),
                ).start()

            @pl.when(bottom & jnp.logical_not(first))
            def _():
                remote(
                    heat.at[pl.ds(per * i + g * GROUP, GROUP), 0],
                    field.at[span, ABOVE],
                    edge_send,
                    halo_recv.at[g],
                    at(down, i),
                ).start()

    each(groups, edge_copies)

    lax.fori_loop(1, groups, lambda g, _: (begin(g), 0)[1], 0)

    def begin_second(g):
        for q in (2, 3):
            exchange(q, 1 - edge_row, g * GROUP, GROUP, second_recv.at[g]).start()

    each(groups - 1, begin_second)

    def begin_last(n):
        for q in (2, 3):
            exchange(q, 1 - edge_row, tail + n, 1, second_recv.at[groups - 1 + n]).start()

    each(GROUP, begin_last)

    arrived(lower.at[:, 0, cut], low_recv)
    part = remote(
        lower.at[:, 0, cut], lower.at[:, 0, cut], low_send, part_recv, at(v, k ^ 1)
    )
    part.start()
    cot_copy.wait()
    src_copy.wait()
    part.wait_recv()
    shifted_weights(cot, lower, weights, v, peers * 8, width)
    meet(3, depth)

    inner_up = (k < 2) & jnp.logical_not(last)
    inner_down = (k >= 2) & jnp.logical_not(first)

    def forward(g):
        span = some(g * GROUP, GROUP)

        @pl.when(inner_up)
        def _():
            remote(
                field.at[span, 7],
                field.at[span, BELOW],
                halo_send,
                halo_recv.at[g],
                at(up, k),
            ).start()

        @pl.when(inner_down)
        def _():
            remote(
                field.at[span, 0],
                field.at[span, ABOVE],
                halo_send,
                halo_recv.at[g],
                at(down, k),
            ).start()

    relays_up = jnp.logical_not(first)
    relays_down = jnp.logical_not(last)

    def relayed(slot):
        c = x + RING * slot
        span = some(c * PIECE, PIECE)
        sem = c * PIECE // GROUP

        @pl.when(relays_up)
        def _():
            arrived(relay.at[0, slot], relay_recv.at[0, slot])
            remote(
                relay.at[0, slot],
                field.at[span, BELOW],
                relay_send.at[0],
                halo_recv.at[sem],
                at(line, k),
            ).start()

        @pl.when(relays_down)
        def _():
            arrived(relay.at[1, slot], relay_recv.at[1, slot])
            remote(
                relay.at[1, slot],
                field.at[span, ABOVE],
                relay_send.at[1],
                halo_recv.at[sem],
                at(line + RING - 1, k),
            ).start()

    for g in range(groups):
        if g == groups - 1:
            relayed(0)
        arrived(field.at[some(g * GROUP, GROUP), 0:2], first_recv.at[g])
        forward(g)
        if g % 2 == 1:
            meet(4 + g // 2, depth)

    own.wait()
    lane = lax.broadcasted_iota(jnp.int32, (1, LANES), 1)
    base = v * (8 * width)

    def group(g, sums):
        span = some(g * GROUP, GROUP)

        @pl.when(g == 1)
        def _():
            relayed(1)

        arrived(field.at[span, 0:2], halo_recv.at[g])
        only = g < groups - 1

        @pl.when(only)
        def _():
            arrived(field.at[span, 0:2], second_recv.at[g])

        def one(s, sums):
            @pl.when(jnp.logical_not(only))
            def _():
                arrived(field.at[pl.ds(s, 1), 0:2], second_recv.at[groups - 1 + s - tail])

            acc = field_defect(
                field,
                weights,
                out,
                s,
                sources[per * k + s] - base,
                amplitude,
                width,
            )
            total = jnp.sum(acc, axis=(0, 1), keepdims=True)
            return sums + jnp.where(lane == s, total, 0.0)

        return lax.fori_loop(g * GROUP, (g + 1) * GROUP, one, sums)

    sums = lax.fori_loop(0, groups, group, jnp.zeros((1, LANES), F32))

    row[...] = sums

    def tell(n, _):
        i = 1 + lax.rem(peers // 2 + TELL * n, peers - 1)
        for step in range(TELL):
            i_step = lax.rem(i + step - 1, peers - 1) + 1
            remote(
                row, rows.at[i_step], sum_send, sum_recv, at(lax.rem(v + i_step, peers), k)
            ).start()
        return 0

    lax.fori_loop(0, (peers - 1) // TELL, tell, 0)

    arrived(lower.at[:, 0], low_send)
    arrived(field.at[0 : 3 * per // 4, 0:8], send)

    inner = (top & jnp.logical_not(last)) | (bottom & jnp.logical_not(first))

    @pl.when(split)
    def _():
        arrived(field.at[:, 0:3], edge_send)

    @pl.when(helps | inner)
    def _():
        arrived(field.at[:, 0:2], edge_send)

    @pl.when(inner_up | inner_down)
    def _():
        arrived(field.at[:, 0:1], halo_send)

    @pl.when(relays_up)
    def _():
        arrived(relay.at[0], relay_send.at[0])

    @pl.when(relays_down)
    def _():
        arrived(relay.at[1], relay_send.at[1])

    arrived(rows.at[1:peers], sum_recv)
    sums = sums + jnp.sum(rows[1:peers], axis=0)
    norms[...] = jnp.sqrt(sums / (peers * 8 * width) + 1e-06)
    arrived(rows.at[1:peers], sum_send)


def scale(defect, norms, out, held, sem):
    per = defect.shape[0]
    lane = lax.broadcasted_iota(jnp.int32, (per, per), 1)
    which = lax.broadcasted_iota(jnp.int32, (per, per), 0)
    own = jnp.where(lane == which, norms[...][None, :], 0.0)
    inverse = 1.0 / jnp.sum(own, axis=1, keepdims=True)
    copies = []
    for s in range(per):
        held[s] = defect[s] * inverse[s : s + 1]
        copies.append(pltpu.make_async_copy(held.at[s], out.at[s], sem.at[s]))
        copies[-1].start()
    for copy in copies:
        copy.wait()


def on_device(heat, cotan, source_index):
    peers = lax.axis_size("vtx")
    rows_dev, width = cotan.shape[1:]
    per = heat.shape[0] // lax.axis_size("src")
    groups, slots = per // GROUP, per // PIECE // RING
    amplitude = math.sqrt(rows_dev * peers * width) / 8.0
    dma, vmem = pltpu.SemaphoreType.DMA, pltpu.VMEM
    anywhere = pl.BlockSpec(memory_space=pl.ANY)
    held = pl.BlockSpec(memory_space=pltpu.VMEM)
    block = jax.ShapeDtypeStruct((per, rows_dev, width), F32)
    defect, norms = pl.pallas_call(
        functools.partial(kernel, peers, amplitude),
        name="defect",
        out_shape=(block, jax.ShapeDtypeStruct((1, LANES), F32)),
        in_specs=[anywhere] * 3,
        out_specs=(held, held),
        scratch_shapes=[
            vmem((4, rows_dev, width), F32),
            pltpu.SMEM(source_index.shape, jnp.int32),
            vmem((per, 2 * rows_dev, width), F32),
            vmem((2, 8, width), F32),
            vmem((7, rows_dev, width), F32),
            vmem((2, slots, PIECE, width), F32),
            vmem((1, LANES), F32),
            vmem((peers, 1, LANES), F32),
            vmem((per, width), F32),
            pltpu.SemaphoreType.REGULAR((6,)),
            *[dma] * 8,
            dma((groups,)),
            dma,
            dma((groups - 1 + GROUP,)),
            dma,
            dma,
            dma((groups,)),
            dma((2,)),
            dma((2, slots)),
            dma,
            dma,
        ],
        compiler_params=pltpu.CompilerParams(
            collective_id=0, has_side_effects=True, vmem_limit_bytes=40 << 20
        ),
        cost_estimate=pl.CostEstimate(
            flops=200_000_000, bytes_accessed=16_000_000, transcendentals=0
        ),
    )(
        *(
            pltpu.with_memory_space_constraint(a, pltpu.HBM)
            for a in (heat, cotan, source_index)
        )
    )
    norms = norms[0, :per]
    normalised = pl.pallas_call(
        scale,
        name="scale",
        out_shape=block,
        in_specs=[held, held],
        out_specs=anywhere,
        scratch_shapes=[vmem(block.shape, F32), dma((per,))],
        compiler_params=pltpu.CompilerParams(vmem_limit_bytes=16 << 20),
        cost_estimate=pl.CostEstimate(
            flops=4_000_000, bytes_accessed=8_400_000, transcendentals=0
        ),
    )(defect, norms)
    return (normalised, norms)


def solution(mesh):
    return jax.shard_map(
        on_device,
        mesh=mesh,
        in_specs=(P(None, ("vtx", "src"), None), P(None, "vtx", None), P()),
        out_specs=(P("src", "vtx", None), P("src")),
        check_vma=False,
    )
```

```python
import functools
import math

import jax
import jax.numpy as jnp
from jax import lax
from jax.experimental import pallas as pl
from jax.experimental.pallas import tpu as pltpu
from jax.sharding import PartitionSpec as P

MESH = pl.DeviceIdType.MESH
RING = 4
PLANE = 8
GROUP = 4
PIECE = 2
TELL = 9
LANES = 128
F32 = jnp.float32
ABOVE, BELOW = 8, 15


def at(v, k):
    return {"vtx": v, "src": k}


def remote(src, dst, send, recv, target):
    return pltpu.make_async_remote_copy(
        src_ref=src,
        dst_ref=dst,
        send_sem=send,
        recv_sem=recv,
        device_id=target,
        device_id_type=MESH,
    )


def signal(sem, target):
    pl.semaphore_signal(sem, inc=1, device_id=target, device_id_type=MESH)


def each(count, body):
    lax.fori_loop(0, count, lambda i, _: (body(i), 0)[1], 0)


def shifted_weights(cot, lower, weights, v, total_rows, width):
    tiles = width // LANES
    step = 8
    lane = lax.broadcasted_iota(jnp.int32, (8, LANES), 1)
    sub = lax.broadcasted_iota(jnp.int32, (8, LANES), 0)
    in_row = sub + 8 * v < total_rows - 1
    has_lower = jnp.full((8, LANES), v, jnp.int32) > 0
    zero = jnp.zeros((8, LANES), F32)

    def block(b, carry):
        for i in range(step):
            j = b * step + i
            cols = pl.ds(pl.multiple_of(j * LANES, LANES), LANES)
            in_col = lane + j * LANES < width - 1
            east = jnp.where(in_col, cot[1, :, cols], 0.0)
            north = jnp.where(in_row, cot[2, :, cols], 0.0)
            diag = jnp.where(in_col & in_row, cot[3, :, cols], 0.0)
            low_n = jnp.where(has_lower, lower[0, :, cols], 0.0)
            low_d = jnp.where(has_lower & in_col, lower[1, :, cols], 0.0)
            south = jnp.where(sub == 0, low_n, pltpu.roll(north, 1, 0))
            diag_s = jnp.where(sub == 0, low_d, pltpu.roll(diag, 1, 0))
            turned = tuple(pltpu.roll(w, 1, 1) for w in (east, diag, diag_s))
            west, diag_w, southwest = (
                jnp.where(lane == 0, left, here) for left, here in zip(carry, turned)
            )
            weights[0, :, cols] = (
                cot[0, :, cols] + east + west + north + south + diag + southwest
            )
            weights[1, :, cols] = north
            weights[2, :, cols] = south
            weights[3, :, cols] = east
            weights[4, :, cols] = west
            weights[5, :, cols] = diag_w
            weights[6, :, cols] = diag_s
            carry = turned
        return carry

    lax.fori_loop(0, tiles // step, block, (zero, zero, zero))


def field_defect(field, weights, out, s, where, amplitude, width):
    lane = lax.broadcasted_iota(jnp.int32, (8, LANES), 1)
    sub = lax.broadcasted_iota(jnp.int32, (8, LANES), 0)
    spot = where - (sub * width + lane)
    zero = jnp.zeros((8, LANES), F32)
    sums = [zero, zero]
    partial, east_at, west_at = None, None, zero

    def finish(j, to_left):
        done = partial - jnp.where(lane == LANES - 1, to_left, east_at)
        out[s, :, j * LANES : (j + 1) * LANES] = done
        sums[j % 2] = sums[j % 2] + done * done

    tiles = width // LANES
    for j in range(tiles):
        cols = slice(j * LANES, (j + 1) * LANES)
        h = field[s, 0:8, cols]
        halo = field[s, 8:16, cols]
        above = pltpu.roll(jnp.where(sub == 0, halo, h), 7, 0)
        below = pltpu.roll(jnp.where(sub == 7, halo, h), 1, 0)
        to_left = weights[4, :, cols] * h + weights[5, :, cols] * above
        to_right = weights[3, :, cols] * h + weights[6, :, cols] * below
        to_left = pltpu.roll(to_left, LANES - 1, 1)
        to_right = pltpu.roll(to_right, 1, 1)
        if j > 0:
            finish(j - 1, to_left)
        partial = (
            weights[0, :, cols] * h
            - weights[1, :, cols] * above
            - weights[2, :, cols] * below
            - jnp.where(lane == 0, west_at, to_right)
            - jnp.where(spot == j * LANES, amplitude, 0.0)
        )
        east_at, west_at = to_left, to_right
    finish(tiles - 1, zero)
    return sums[0] + sums[1]


def kernel(
    peers,
    amplitude,
    heat,
    cot_hbm,
    sources_hbm,
    out,
    norms,
    cot,
    sources,
    field,
    lower,
    weights,
    relay,
    row,
    rows,
    spare,
    stage,
    known,
    stage_sem,
    own_sem,
    cot_sem,
    src_sem,
    low_send,
    low_recv,
    part_recv,
    hand_recv,
    send,
    first_recv,
    near_recv,
    second_recv,
    edge_send,
    halo_send,
    halo_recv,
    relay_send,
    relay_recv,
    sum_send,
    sum_recv,
):
    v, k = lax.axis_index("vtx"), lax.axis_index("src")
    x = lax.rem(v, RING)
    per, _, width = field.shape
    groups, pieces = per // GROUP, per // PIECE
    tail = per - GROUP
    up, down = lax.rem(v + 1, peers), lax.rem(v + peers - 1, peers)
    line = v - x
    top, bottom = k == 3, k == 0
    last, first = x == RING - 1, x == 0

    around = [line + lax.rem(x + i, RING) for i in range(1, RING)]
    across = v + RING - 2 * RING * lax.rem(v // RING, 2)
    depth = [lax.rem(v + PLANE, peers), lax.rem(v + peers - PLANE, peers)]
    shared = [at(v, k ^ q) for q in (2, 3, 1)]
    around, across, depth = (
        [at(i, k) for i in around],
        [at(across, k)],
        [at(i, k) for i in depth],
    )

    barrier = pltpu.get_barrier_semaphore()
    near = shared + around + across + depth
    for target in near:
        signal(barrier, target)
    other = [2 - 2 * (k // 2) + core for core in range(2)]
    edge_row = jnp.where(top, 1, 0)
    staged = [
        pltpu.make_async_copy(
            heat.at[pl.ds(per * to, GROUP), edge_row], stage.at[i], stage_sem.at[i]
        )
        for i, to in enumerate(other)
    ]
    for copy in staged:
        copy.start()
    cot_copy = pltpu.make_async_copy(cot_hbm, cot, cot_sem)
    cot_copy.start()
    src_copy = pltpu.make_async_copy(sources_hbm, sources, src_sem)
    src_copy.start()
    own = pltpu.make_async_copy(
        heat.at[pl.ds(per * k, per)],
        field.at[:, pl.ds(pl.multiple_of(2 * k, 2), 2)],
        own_sem,
    )
    own.start()
    pl.semaphore_wait(barrier, len(near))

    def some(start, count):
        return pl.ds(start, count)

    def arrived(ref, sem):
        pltpu.make_async_copy(ref, ref, sem).wait()

    def exchange(to, r, start, count, sem):
        return remote(
            heat.at[pl.ds(per * to + start, count), r],
            field.at[some(start, count), 2 * k + r],
            send,
            sem,
            at(v, to),
        )

    def begin(g):
        for to in other:
            exchange(to, edge_row, g * GROUP, GROUP, first_recv.at[g]).start()

    for i, to in enumerate(other):
        staged[i].wait()
        remote(
            stage.at[i],
            field.at[0:GROUP, 2 * k + edge_row],
            send,
            first_recv.at[0],
            at(v, to),
        ).start()

    above_side = last & (k >= 2)
    below_side = first & (k < 2)
    holds = top | bottom
    own_row = jnp.where(top, 1, 0)
    block_row = jnp.where(k >= 2, 7, 0)
    split = (above_side | below_side) & holds
    helps = (above_side | below_side) & jnp.logical_not(holds)
    handed = remote(
        heat.at[pl.ds(per * (k ^ 3), per), own_row],
        spare,
        edge_send,
        hand_recv,
        at(v, k ^ 1),
    )

    @pl.when(split)
    def _():
        handed.start()

    def begin_near(g):
        remote(
            heat.at[pl.ds(per * (k ^ 1) + g * GROUP, GROUP)],
            field.at[some(g * GROUP, GROUP), pl.ds(pl.multiple_of(2 * k, 2), 2)],
            send,
            near_recv,
            at(v, k ^ 1),
        ).start()

    each(groups, begin_near)

    def meet(stage, targets):
        for target in targets:
            signal(known.at[stage], target)
        pl.semaphore_wait(known.at[stage], len(targets))

    meet(0, around)
    meet(1, across)
    meet(2, shared)

    half = width // 2
    cut = pl.ds(pl.multiple_of(lax.rem(k, 2) * half, half), half)
    low = remote(
        cot_hbm.at[pl.ds(2, 2), 7, cut],
        lower.at[:, 0, cut],
        low_send,
        low_recv,
        at(up, k),
    )
    low.start()

    arrived(field.at[:, 0:2], near_recv)

    @pl.when(helps)
    def _():
        handed.wait_recv()

    def wrap_copies(c):
        via = lax.rem(c, RING)
        slot = c // RING
        span = some(c * PIECE, PIECE)
        sem = c * PIECE // GROUP

        def send_on(src, m):
            for side, active, end, hop in (
                (0, above_side, 0, up),
                (1, below_side, RING - 1, down - (RING - 1)),
            ):

                @pl.when(active & (via == end))
                def _():
                    remote(
                        src,
                        field.at[span, (BELOW, ABOVE)[side]],
                        edge_send,
                        halo_recv.at[sem],
                        at(hop + via, m),
                    ).start()

                @pl.when(active & (via != end))
                def _():
                    remote(
                        src,
                        relay.at[side, slot],
                        edge_send,
                        relay_recv.at[side, slot],
                        at(hop + via, m),
                    ).start()

        @pl.when(split)
        def _():
            for m in (k, k ^ 2):
                send_on(heat.at[pl.ds(per * m + c * PIECE, PIECE), own_row], m)

        @pl.when(helps)
        def _():
            send_on(field.at[span, block_row], k)
            send_on(spare.at[span], k ^ 2)

    each(pieces, wrap_copies)

    def edge_copies(g):
        span = some(g * GROUP, GROUP)
        for i in range(2):

            @pl.when(top & jnp.logical_not(last))
            def _():
                m = 2 + i
                remote(
                    heat.at[pl.ds(per * m + g * GROUP, GROUP), 1],
                    field.at[span, BELOW],
                    edge_send,
                    halo_recv.at[g],
                    at(up, m),
                ).start()

            @pl.when(bottom & jnp.logical_not(first))
            def _():
                remote(
                    heat.at[pl.ds(per * i + g * GROUP, GROUP), 0],
                    field.at[span, ABOVE],
                    edge_send,
                    halo_recv.at[g],
                    at(down, i),
                ).start()

    each(groups, edge_copies)

    lax.fori_loop(1, groups, lambda g, _: (begin(g), 0)[1], 0)

    def begin_second(g):
        for to in other:
            exchange(to, 1 - edge_row, g * GROUP, GROUP, second_recv.at[g]).start()

    each(groups - 1, begin_second)

    def begin_last(n, to):
        exchange(to, 1 - edge_row, tail + n, 1, second_recv.at[groups - 1 + n]).start()

    for to in other:
        for n in range(GROUP):
            begin_last(n, to)

    arrived(lower.at[:, 0, cut], low_recv)
    part = remote(
        lower.at[:, 0, cut], lower.at[:, 0, cut], low_send, part_recv, at(v, k ^ 1)
    )
    part.start()
    cot_copy.wait()
    src_copy.wait()
    part.wait_recv()
    shifted_weights(cot, lower, weights, v, peers * 8, width)
    meet(3, depth)

    inner_up = (k < 2) & jnp.logical_not(last)
    inner_down = (k >= 2) & jnp.logical_not(first)

    def forward(g):
        span = some(g * GROUP, GROUP)

        @pl.when(inner_up)
        def _():
            remote(
                field.at[span, 7],
                field.at[span, BELOW],
                halo_send,
                halo_recv.at[g],
                at(up, k),
            ).start()

        @pl.when(inner_down)
        def _():
            remote(
                field.at[span, 0],
                field.at[span, ABOVE],
                halo_send,
                halo_recv.at[g],
                at(down, k),
            ).start()

    relays_up = jnp.logical_not(first)
    relays_down = jnp.logical_not(last)

    def relayed(slot):
        c = x + RING * slot
        span = some(c * PIECE, PIECE)
        sem = c * PIECE // GROUP

        @pl.when(relays_up)
        def _():
            arrived(relay.at[0, slot], relay_recv.at[0, slot])
            remote(
                relay.at[0, slot],
                field.at[span, BELOW],
                relay_send.at[0],
                halo_recv.at[sem],
                at(line, k),
            ).start()

        @pl.when(relays_down)
        def _():
            arrived(relay.at[1, slot], relay_recv.at[1, slot])
            remote(
                relay.at[1, slot],
                field.at[span, ABOVE],
                relay_send.at[1],
                halo_recv.at[sem],
                at(line + RING - 1, k),
            ).start()

    for g in range(groups):
        if g == groups - 1:
            relayed(0)
        arrived(field.at[some(g * GROUP, GROUP), 0:2], first_recv.at[g])
        forward(g)
        if g % 2 == 1:
            meet(4 + g // 2, depth)

    own.wait()
    lane = lax.broadcasted_iota(jnp.int32, (1, LANES), 1)
    base = v * (8 * width)

    def group(g, sums):
        span = some(g * GROUP, GROUP)

        @pl.when(g == 1)
        def _():
            relayed(1)

        arrived(field.at[span, 0:2], halo_recv.at[g])
        only = g < groups - 1

        @pl.when(only)
        def _():
            arrived(field.at[span, 0:2], second_recv.at[g])

        def one(s, sums):
            @pl.when(jnp.logical_not(only))
            def _():
                arrived(field.at[pl.ds(s, 1), 0:2], second_recv.at[groups - 1 + s - tail])

            acc = field_defect(
                field,
                weights,
                out,
                s,
                sources[per * k + s] - base,
                amplitude,
                width,
            )
            total = jnp.sum(acc, axis=(0, 1), keepdims=True)
            return sums + jnp.where(lane == s, total, 0.0)

        return lax.fori_loop(g * GROUP, (g + 1) * GROUP, one, sums)

    sums = lax.fori_loop(0, groups, group, jnp.zeros((1, LANES), F32))

    row[...] = sums

    def tell(n, _):
        far = peers // 2 + PLANE - 1
        for step in range(TELL):
            i_step = 1 + lax.rem(far + peers - 2 - TELL * n - step, peers - 1)
            remote(
                row, rows.at[i_step], sum_send, sum_recv, at(lax.rem(v + i_step, peers), k)
            ).start()
        return 0

    lax.fori_loop(0, (peers - 1) // TELL, tell, 0)

    arrived(lower.at[:, 0], low_send)
    arrived(field.at[0 : 3 * per // 4, 0:8], send)

    inner = (top & jnp.logical_not(last)) | (bottom & jnp.logical_not(first))

    @pl.when(split)
    def _():
        arrived(field.at[:, 0:3], edge_send)

    @pl.when(helps | inner)
    def _():
        arrived(field.at[:, 0:2], edge_send)

    @pl.when(inner_up | inner_down)
    def _():
        arrived(field.at[:, 0:1], halo_send)

    @pl.when(relays_up)
    def _():
        arrived(relay.at[0], relay_send.at[0])

    @pl.when(relays_down)
    def _():
        arrived(relay.at[1], relay_send.at[1])

    arrived(rows.at[1:peers], sum_recv)
    sums = sums + jnp.sum(rows[1:peers], axis=0)
    norms[...] = jnp.sqrt(sums / (peers * 8 * width) + 1e-06)
    arrived(rows.at[1:peers], sum_send)


def scale(defect, norms, out, held, sem):
    per = defect.shape[0]
    lane = lax.broadcasted_iota(jnp.int32, (per, per), 1)
    which = lax.broadcasted_iota(jnp.int32, (per, per), 0)
    own = jnp.where(lane == which, norms[...][None, :], 0.0)
    inverse = 1.0 / jnp.sum(own, axis=1, keepdims=True)
    copies = []
    for s in range(per):
        held[s] = defect[s] * inverse[s : s + 1]
        copies.append(pltpu.make_async_copy(held.at[s], out.at[s], sem.at[s]))
        copies[-1].start()
    for copy in copies:
        copy.wait()


def on_device(heat, cotan, source_index):
    peers = lax.axis_size("vtx")
    rows_dev, width = cotan.shape[1:]
    per = heat.shape[0] // lax.axis_size("src")
    groups, slots = per // GROUP, per // PIECE // RING
    amplitude = math.sqrt(rows_dev * peers * width) / 8.0
    dma, vmem = pltpu.SemaphoreType.DMA, pltpu.VMEM
    anywhere = pl.BlockSpec(memory_space=pl.ANY)
    held = pl.BlockSpec(memory_space=pltpu.VMEM)
    block = jax.ShapeDtypeStruct((per, rows_dev, width), F32)
    defect, norms = pl.pallas_call(
        functools.partial(kernel, peers, amplitude),
        name="defect",
        out_shape=(block, jax.ShapeDtypeStruct((1, LANES), F32)),
        in_specs=[anywhere] * 3,
        out_specs=(held, held),
        scratch_shapes=[
            vmem((4, rows_dev, width), F32),
            pltpu.SMEM(source_index.shape, jnp.int32),
            vmem((per, 2 * rows_dev, width), F32),
            vmem((2, 8, width), F32),
            vmem((7, rows_dev, width), F32),
            vmem((2, slots, PIECE, width), F32),
            vmem((1, LANES), F32),
            vmem((peers, 1, LANES), F32),
            vmem((per, width), F32),
            vmem((2, GROUP, width), F32),
            pltpu.SemaphoreType.REGULAR((6,)),
            dma((2,)),
            *[dma] * 8,
            dma((groups,)),
            dma,
            dma((groups - 1 + GROUP,)),
            dma,
            dma,
            dma((groups,)),
            dma((2,)),
            dma((2, slots)),
            dma,
            dma,
        ],
        compiler_params=pltpu.CompilerParams(
            collective_id=0, has_side_effects=True, vmem_limit_bytes=40 << 20
        ),
        cost_estimate=pl.CostEstimate(
            flops=200_000_000, bytes_accessed=16_000_000, transcendentals=0
        ),
    )(
        *(
            pltpu.with_memory_space_constraint(a, pltpu.HBM)
            for a in (heat, cotan, source_index)
        )
    )
    norms = norms[0, :per]
    normalised = pl.pallas_call(
        scale,
        name="scale",
        out_shape=block,
        in_specs=[held, held],
        out_specs=anywhere,
        scratch_shapes=[vmem(block.shape, F32), dma((per,))],
        compiler_params=pltpu.CompilerParams(vmem_limit_bytes=16 << 20),
        cost_estimate=pl.CostEstimate(
            flops=4_000_000, bytes_accessed=8_400_000, transcendentals=0
        ),
    )(defect, norms)
    return (normalised, norms)


def solution(mesh):
    return jax.shard_map(
        on_device,
        mesh=mesh,
        in_specs=(P(None, ("vtx", "src"), None), P(None, "vtx", None), P()),
        out_specs=(P("src", "vtx", None), P("src")),
        check_vma=False,
    )
```

```python
import functools
import math

import jax
import jax.numpy as jnp
from jax import lax
from jax.experimental import pallas as pl
from jax.experimental.pallas import tpu as pltpu
from jax.sharding import PartitionSpec as P

MESH = pl.DeviceIdType.MESH
RING = 4
PLANE = 8
GROUP = 4
PIECE = 2
STOPS = (0, 1, 3, 6, 9, 12, 15)
TELL = 9
LANES = 128
F32 = jnp.float32
ABOVE, BELOW = 8, 15


def at(v, k):
    return {"vtx": v, "src": k}


def remote(src, dst, send, recv, target):
    return pltpu.make_async_remote_copy(
        src_ref=src,
        dst_ref=dst,
        send_sem=send,
        recv_sem=recv,
        device_id=target,
        device_id_type=MESH,
    )


def signal(sem, target):
    pl.semaphore_signal(sem, inc=1, device_id=target, device_id_type=MESH)


def each(count, body):
    lax.fori_loop(0, count, lambda i, _: (body(i), 0)[1], 0)


def shifted_weights(cot, lower, weights, v, total_rows, width):
    tiles = width // LANES
    step = 8
    lane = lax.broadcasted_iota(jnp.int32, (8, LANES), 1)
    sub = lax.broadcasted_iota(jnp.int32, (8, LANES), 0)
    in_row = sub + 8 * v < total_rows - 1
    has_lower = jnp.full((8, LANES), v, jnp.int32) > 0
    zero = jnp.zeros((8, LANES), F32)

    def block(b, carry):
        for i in range(step):
            j = b * step + i
            cols = pl.ds(pl.multiple_of(j * LANES, LANES), LANES)
            in_col = lane + j * LANES < width - 1
            east = jnp.where(in_col, cot[1, :, cols], 0.0)
            north = jnp.where(in_row, cot[2, :, cols], 0.0)
            diag = jnp.where(in_col & in_row, cot[3, :, cols], 0.0)
            low_n = jnp.where(has_lower, lower[0, :, cols], 0.0)
            low_d = jnp.where(has_lower & in_col, lower[1, :, cols], 0.0)
            south = jnp.where(sub == 0, low_n, pltpu.roll(north, 1, 0))
            diag_s = jnp.where(sub == 0, low_d, pltpu.roll(diag, 1, 0))
            turned = tuple(pltpu.roll(w, 1, 1) for w in (east, diag, diag_s))
            west, diag_w, southwest = (
                jnp.where(lane == 0, left, here) for left, here in zip(carry, turned)
            )
            weights[0, :, cols] = (
                cot[0, :, cols] + east + west + north + south + diag + southwest
            )
            weights[1, :, cols] = north
            weights[2, :, cols] = south
            weights[3, :, cols] = east
            weights[4, :, cols] = west
            weights[5, :, cols] = diag_w
            weights[6, :, cols] = diag_s
            carry = turned
        return carry

    lax.fori_loop(0, tiles // step, block, (zero, zero, zero))


def field_defect(field, weights, out, s, where, amplitude, width):
    lane = lax.broadcasted_iota(jnp.int32, (8, LANES), 1)
    sub = lax.broadcasted_iota(jnp.int32, (8, LANES), 0)
    spot = where - (sub * width + lane)
    zero = jnp.zeros((8, LANES), F32)
    sums = [zero, zero]
    partial, east_at, west_at = None, None, zero

    def finish(j, to_left):
        done = partial - jnp.where(lane == LANES - 1, to_left, east_at)
        out[s, :, j * LANES : (j + 1) * LANES] = done
        sums[j % 2] = sums[j % 2] + done * done

    tiles = width // LANES
    for j in range(tiles):
        cols = slice(j * LANES, (j + 1) * LANES)
        h = field[s, 0:8, cols]
        halo = field[s, 8:16, cols]
        above = pltpu.roll(jnp.where(sub == 0, halo, h), 7, 0)
        below = pltpu.roll(jnp.where(sub == 7, halo, h), 1, 0)
        to_left = weights[4, :, cols] * h + weights[5, :, cols] * above
        to_right = weights[3, :, cols] * h + weights[6, :, cols] * below
        to_left = pltpu.roll(to_left, LANES - 1, 1)
        to_right = pltpu.roll(to_right, 1, 1)
        if j > 0:
            finish(j - 1, to_left)
        partial = (
            weights[0, :, cols] * h
            - weights[1, :, cols] * above
            - weights[2, :, cols] * below
            - jnp.where(lane == 0, west_at, to_right)
            - jnp.where(spot == j * LANES, amplitude, 0.0)
        )
        east_at, west_at = to_left, to_right
    finish(tiles - 1, zero)
    return sums[0] + sums[1]


def kernel(
    peers,
    amplitude,
    heat,
    cot_hbm,
    sources_hbm,
    out,
    norms,
    cot,
    sources,
    field,
    lower,
    weights,
    relay,
    row,
    rows,
    spare,
    stage,
    known,
    stage_sem,
    own_sem,
    cot_sem,
    src_sem,
    low_send,
    low_recv,
    part_recv,
    hand_recv,
    send,
    first_recv,
    near_recv,
    second_recv,
    edge_send,
    halo_send,
    halo_recv,
    relay_send,
    relay_recv,
    sum_send,
    sum_recv,
):
    v, k = lax.axis_index("vtx"), lax.axis_index("src")
    x = lax.rem(v, RING)
    per, _, width = field.shape
    groups, pieces = per // GROUP, per // PIECE
    tail = per - GROUP
    up, down = lax.rem(v + 1, peers), lax.rem(v + peers - 1, peers)
    line = v - x
    top, bottom = k == 3, k == 0
    last, first = x == RING - 1, x == 0

    around = [line + lax.rem(x + i, RING) for i in range(1, RING)]
    across = v + RING - 2 * RING * lax.rem(v // RING, 2)
    depth = [lax.rem(v + PLANE, peers), lax.rem(v + peers - PLANE, peers)]
    shared = [at(v, k ^ q) for q in (2, 3, 1)]
    around, across, depth = (
        [at(i, k) for i in around],
        [at(across, k)],
        [at(i, k) for i in depth],
    )

    barrier = pltpu.get_barrier_semaphore()
    near = shared + around + across + depth
    for target in near:
        signal(barrier, target)
    other = [2 - 2 * (k // 2) + core for core in (1, 0)]
    edge_row = jnp.where(top, 1, 0)
    staged = [
        pltpu.make_async_copy(
            heat.at[pl.ds(per * to, GROUP), edge_row], stage.at[i], stage_sem.at[i]
        )
        for i, to in enumerate(other)
    ]
    for copy in staged:
        copy.start()
    cot_copy = pltpu.make_async_copy(cot_hbm, cot, cot_sem)
    cot_copy.start()
    src_copy = pltpu.make_async_copy(sources_hbm, sources, src_sem)
    src_copy.start()
    own = pltpu.make_async_copy(
        heat.at[pl.ds(per * k, per)],
        field.at[:, pl.ds(pl.multiple_of(2 * k, 2), 2)],
        own_sem,
    )
    own.start()
    pl.semaphore_wait(barrier, len(near))

    def some(start, count):
        return pl.ds(start, count)

    def arrived(ref, sem):
        pltpu.make_async_copy(ref, ref, sem).wait()

    def exchange(to, r, start, count, sem):
        return remote(
            heat.at[pl.ds(per * to + start, count), r],
            field.at[some(start, count), 2 * k + r],
            send,
            sem,
            at(v, to),
        )

    def begin(g):
        for to in other:
            exchange(to, edge_row, g * GROUP, GROUP, first_recv.at[g]).start()

    for i, to in enumerate(other):
        staged[i].wait()
        remote(
            stage.at[i],
            field.at[0:GROUP, 2 * k + edge_row],
            send,
            first_recv.at[0],
            at(v, to),
        ).start()

    above_side = last & (k >= 2)
    below_side = first & (k < 2)
    holds = top | bottom
    own_row = jnp.where(top, 1, 0)
    block_row = jnp.where(k >= 2, 7, 0)
    split = (above_side | below_side) & holds
    helps = (above_side | below_side) & jnp.logical_not(holds)
    handed = remote(
        heat.at[pl.ds(per * (k ^ 3), per), own_row],
        spare,
        edge_send,
        hand_recv,
        at(v, k ^ 1),
    )

    @pl.when(split)
    def _():
        handed.start()

    def begin_near(g):
        remote(
            heat.at[pl.ds(per * (k ^ 1) + g * GROUP, GROUP)],
            field.at[some(g * GROUP, GROUP), pl.ds(pl.multiple_of(2 * k, 2), 2)],
            send,
            near_recv,
            at(v, k ^ 1),
        ).start()

    each(groups, begin_near)

    def meet(stage, targets):
        for target in targets:
            signal(known.at[stage], target)
        pl.semaphore_wait(known.at[stage], len(targets))

    meet(0, around)
    meet(1, across)
    meet(2, shared)

    half = width // 2
    cut = pl.ds(pl.multiple_of(lax.rem(k, 2) * half, half), half)
    low = remote(
        cot_hbm.at[pl.ds(2, 2), 7, cut],
        lower.at[:, 0, cut],
        low_send,
        low_recv,
        at(up, k),
    )
    low.start()

    arrived(field.at[:, 0:2], near_recv)

    @pl.when(helps)
    def _():
        handed.wait_recv()

    def wrap_copies(c):
        via = lax.rem(c, RING)
        slot = c // RING
        span = some(c * PIECE, PIECE)
        sem = c * PIECE // GROUP

        def send_on(src, m):
            for side, active, end, hop in (
                (0, above_side, 0, up),
                (1, below_side, RING - 1, down - (RING - 1)),
            ):

                @pl.when(active & (via == end))
                def _():
                    remote(
                        src,
                        field.at[span, (BELOW, ABOVE)[side]],
                        edge_send,
                        halo_recv.at[sem],
                        at(hop + via, m),
                    ).start()

                @pl.when(active & (via != end))
                def _():
                    remote(
                        src,
                        relay.at[side, slot],
                        edge_send,
                        relay_recv.at[side, slot],
                        at(hop + via, m),
                    ).start()

        @pl.when(split)
        def _():
            for m in (k, k ^ 2):
                send_on(heat.at[pl.ds(per * m + c * PIECE, PIECE), own_row], m)

        @pl.when(helps)
        def _():
            send_on(field.at[span, block_row], k)
            send_on(spare.at[span], k ^ 2)

    each(pieces, wrap_copies)

    def edge_copies(g):
        span = some(g * GROUP, GROUP)
        for i in range(2):

            @pl.when(top & jnp.logical_not(last))
            def _():
                m = 2 + i
                remote(
                    heat.at[pl.ds(per * m + g * GROUP, GROUP), 1],
                    field.at[span, BELOW],
                    edge_send,
                    halo_recv.at[g],
                    at(up, m),
                ).start()

            @pl.when(bottom & jnp.logical_not(first))
            def _():
                remote(
                    heat.at[pl.ds(per * i + g * GROUP, GROUP), 0],
                    field.at[span, ABOVE],
                    edge_send,
                    halo_recv.at[g],
                    at(down, i),
                ).start()

    each(groups, edge_copies)

    lax.fori_loop(1, groups, lambda g, _: (begin(g), 0)[1], 0)

    def begin_second(g):
        for to in other:
            exchange(to, 1 - edge_row, g * GROUP, GROUP, second_recv.at[g]).start()

    each(groups - 1, begin_second)

    def begin_last(n, to):
        exchange(to, 1 - edge_row, tail + n, 1, second_recv.at[groups - 1 + n]).start()

    for n in range(GROUP - 2):
        for to in other:
            begin_last(n, to)
    for to in other:
        for n in range(GROUP - 2, GROUP):
            begin_last(n, to)

    arrived(lower.at[:, 0, cut], low_recv)
    part = remote(
        lower.at[:, 0, cut], lower.at[:, 0, cut], low_send, part_recv, at(v, k ^ 1)
    )
    part.start()
    cot_copy.wait()
    src_copy.wait()
    part.wait_recv()
    shifted_weights(cot, lower, weights, v, peers * 8, width)
    meet(3, depth)

    inner_up = (k < 2) & jnp.logical_not(last)
    inner_down = (k >= 2) & jnp.logical_not(first)

    def forward(g):
        span = some(g * GROUP, GROUP)

        @pl.when(inner_up)
        def _():
            remote(
                field.at[span, 7],
                field.at[span, BELOW],
                halo_send,
                halo_recv.at[g],
                at(up, k),
            ).start()

        @pl.when(inner_down)
        def _():
            remote(
                field.at[span, 0],
                field.at[span, ABOVE],
                halo_send,
                halo_recv.at[g],
                at(down, k),
            ).start()

    relays_up = jnp.logical_not(first)
    relays_down = jnp.logical_not(last)

    def relayed(slot):
        c = x + RING * slot
        span = some(c * PIECE, PIECE)
        sem = c * PIECE // GROUP

        @pl.when(relays_up)
        def _():
            arrived(relay.at[0, slot], relay_recv.at[0, slot])
            remote(
                relay.at[0, slot],
                field.at[span, BELOW],
                relay_send.at[0],
                halo_recv.at[sem],
                at(line, k),
            ).start()

        @pl.when(relays_down)
        def _():
            arrived(relay.at[1, slot], relay_recv.at[1, slot])
            remote(
                relay.at[1, slot],
                field.at[span, ABOVE],
                relay_send.at[1],
                halo_recv.at[sem],
                at(line + RING - 1, k),
            ).start()

    for g in range(groups):
        if g == groups - 1:
            relayed(0)
        arrived(field.at[some(g * GROUP, GROUP), 0:2], first_recv.at[g])
        forward(g)
        if g % 2 == 1:
            meet(4 + g // 2, depth)

    own.wait()
    lane = lax.broadcasted_iota(jnp.int32, (1, LANES), 1)
    base = v * (8 * width)

    def group(g, sums):
        span = some(g * GROUP, GROUP)

        @pl.when(g == 1)
        def _():
            relayed(1)

        arrived(field.at[span, 0:2], halo_recv.at[g])
        only = g < groups - 1

        @pl.when(only)
        def _():
            arrived(field.at[span, 0:2], second_recv.at[g])

        def one(s, sums):
            @pl.when(jnp.logical_not(only))
            def _():
                arrived(field.at[pl.ds(s, 1), 0:2], second_recv.at[groups - 1 + s - tail])

            acc = field_defect(
                field,
                weights,
                out,
                s,
                sources[per * k + s] - base,
                amplitude,
                width,
            )
            total = jnp.sum(acc, axis=(0, 1), keepdims=True)
            return sums + jnp.where(lane == s, total, 0.0)

        return lax.fori_loop(g * GROUP, (g + 1) * GROUP, one, sums)

    sums = lax.fori_loop(0, groups, group, jnp.zeros((1, LANES), F32))

    row[...] = sums

    def tell(n, _):
        far = peers // 2 + PLANE - 1
        for step in range(TELL):
            i_step = 1 + lax.rem(far + peers - 2 - TELL * n - step, peers - 1)
            remote(
                row, rows.at[i_step], sum_send, sum_recv, at(lax.rem(v + i_step, peers), k)
            ).start()
        return 0

    lax.fori_loop(0, (peers - 1) // TELL, tell, 0)

    arrived(lower.at[:, 0], low_send)
    arrived(field.at[0 : 3 * per // 4, 0:8], send)

    inner = (top & jnp.logical_not(last)) | (bottom & jnp.logical_not(first))

    @pl.when(split)
    def _():
        arrived(field.at[:, 0:3], edge_send)

    @pl.when(helps | inner)
    def _():
        arrived(field.at[:, 0:2], edge_send)

    @pl.when(inner_up | inner_down)
    def _():
        arrived(field.at[:, 0:1], halo_send)

    @pl.when(relays_up)
    def _():
        arrived(relay.at[0], relay_send.at[0])

    @pl.when(relays_down)
    def _():
        arrived(relay.at[1], relay_send.at[1])

    arrived(rows.at[1:peers], sum_recv)
    sums = sums + jnp.sum(rows[1:peers], axis=0)
    norms[...] = jnp.sqrt(sums / (peers * 8 * width) + 1e-06)
    arrived(rows.at[1:peers], sum_send)


def scale(defect, norms, out, held, sem):
    per = defect.shape[0]
    lane = lax.broadcasted_iota(jnp.int32, (per, per), 1)
    which = lax.broadcasted_iota(jnp.int32, (per, per), 0)
    own = jnp.where(lane == which, norms[...][None, :], 0.0)
    inverse = 1.0 / jnp.sum(own, axis=1, keepdims=True)
    copies, begun = [], 0
    for s in range(per):
        held[s] = defect[s] * inverse[s : s + 1]
        if s in STOPS:
            span = pl.ds(begun, s + 1 - begun)
            copies.append(
                pltpu.make_async_copy(held.at[span], out.at[span], sem.at[len(copies)])
            )
            copies[-1].start()
            begun = s + 1
    for copy in copies:
        copy.wait()


def on_device(heat, cotan, source_index):
    peers = lax.axis_size("vtx")
    rows_dev, width = cotan.shape[1:]
    per = heat.shape[0] // lax.axis_size("src")
    groups, slots = per // GROUP, per // PIECE // RING
    amplitude = math.sqrt(rows_dev * peers * width) / 8.0
    dma, vmem = pltpu.SemaphoreType.DMA, pltpu.VMEM
    anywhere = pl.BlockSpec(memory_space=pl.ANY)
    held = pl.BlockSpec(memory_space=pltpu.VMEM)
    block = jax.ShapeDtypeStruct((per, rows_dev, width), F32)
    defect, norms = pl.pallas_call(
        functools.partial(kernel, peers, amplitude),
        name="defect",
        out_shape=(block, jax.ShapeDtypeStruct((1, LANES), F32)),
        in_specs=[anywhere] * 3,
        out_specs=(held, held),
        scratch_shapes=[
            vmem((4, rows_dev, width), F32),
            pltpu.SMEM(source_index.shape, jnp.int32),
            vmem((per, 2 * rows_dev, width), F32),
            vmem((2, 8, width), F32),
            vmem((7, rows_dev, width), F32),
            vmem((2, slots, PIECE, width), F32),
            vmem((1, LANES), F32),
            vmem((peers, 1, LANES), F32),
            vmem((per, width), F32),
            vmem((2, GROUP, width), F32),
            pltpu.SemaphoreType.REGULAR((6,)),
            dma((2,)),
            *[dma] * 8,
            dma((groups,)),
            dma,
            dma((groups - 1 + GROUP,)),
            dma,
            dma,
            dma((groups,)),
            dma((2,)),
            dma((2, slots)),
            dma,
            dma,
        ],
        compiler_params=pltpu.CompilerParams(
            collective_id=0, has_side_effects=True, vmem_limit_bytes=40 << 20
        ),
        cost_estimate=pl.CostEstimate(
            flops=200_000_000, bytes_accessed=16_000_000, transcendentals=0
        ),
    )(
        *(
            pltpu.with_memory_space_constraint(a, pltpu.HBM)
            for a in (heat, cotan, source_index)
        )
    )
    norms = norms[0, :per]
    normalised = pl.pallas_call(
        scale,
        name="scale",
        out_shape=block,
        in_specs=[held, held],
        out_specs=anywhere,
        scratch_shapes=[vmem(block.shape, F32), dma((len(STOPS),))],
        compiler_params=pltpu.CompilerParams(vmem_limit_bytes=16 << 20),
        cost_estimate=pl.CostEstimate(
            flops=4_000_000, bytes_accessed=8_400_000, transcendentals=0
        ),
    )(defect, norms)
    return (normalised, norms)


def solution(mesh):
    return jax.shard_map(
        on_device,
        mesh=mesh,
        in_specs=(P(None, ("vtx", "src"), None), P(None, "vtx", None), P()),
        out_specs=(P("src", "vtx", None), P("src")),
        check_vma=False,
    )
```

```python
import functools
import math

import jax
import jax.numpy as jnp
from jax import lax
from jax.experimental import pallas as pl
from jax.experimental.pallas import tpu as pltpu
from jax.sharding import PartitionSpec as P

MESH = pl.DeviceIdType.MESH
RING = 4
PLANE = 8
GROUP = 4
PIECE = 2
STOPS = (0, 1, 3, 6, 9, 12, 15)
TELL = 9
LANES = 128
F32 = jnp.float32
ABOVE, BELOW = 8, 15


def at(v, k):
    return {"vtx": v, "src": k}


def remote(src, dst, send, recv, target):
    return pltpu.make_async_remote_copy(
        src_ref=src,
        dst_ref=dst,
        send_sem=send,
        recv_sem=recv,
        device_id=target,
        device_id_type=MESH,
    )


def signal(sem, target):
    pl.semaphore_signal(sem, inc=1, device_id=target, device_id_type=MESH)


def each(count, body):
    lax.fori_loop(0, count, lambda i, _: (body(i), 0)[1], 0)


def shifted_weights(cot, lower, weights, v, total_rows, width):
    tiles = width // LANES
    step = 8
    lane = lax.broadcasted_iota(jnp.int32, (8, LANES), 1)
    sub = lax.broadcasted_iota(jnp.int32, (8, LANES), 0)
    in_row = sub + 8 * v < total_rows - 1
    has_lower = jnp.full((8, LANES), v, jnp.int32) > 0
    zero = jnp.zeros((8, LANES), F32)

    def block(b, carry):
        for i in range(step):
            j = b * step + i
            cols = pl.ds(pl.multiple_of(j * LANES, LANES), LANES)
            in_col = lane + j * LANES < width - 1
            east = jnp.where(in_col, cot[1, :, cols], 0.0)
            north = jnp.where(in_row, cot[2, :, cols], 0.0)
            diag = jnp.where(in_col & in_row, cot[3, :, cols], 0.0)
            low_n = jnp.where(has_lower, lower[0, :, cols], 0.0)
            low_d = jnp.where(has_lower & in_col, lower[1, :, cols], 0.0)
            south = jnp.where(sub == 0, low_n, pltpu.roll(north, 1, 0))
            diag_s = jnp.where(sub == 0, low_d, pltpu.roll(diag, 1, 0))
            turned = tuple(pltpu.roll(w, 1, 1) for w in (east, diag, diag_s))
            west, diag_w, southwest = (
                jnp.where(lane == 0, left, here) for left, here in zip(carry, turned)
            )
            weights[0, :, cols] = (
                cot[0, :, cols] + east + west + north + south + diag + southwest
            )
            weights[1, :, cols] = north
            weights[2, :, cols] = south
            weights[3, :, cols] = east
            weights[4, :, cols] = west
            weights[5, :, cols] = diag_w
            weights[6, :, cols] = diag_s
            carry = turned
        return carry

    lax.fori_loop(0, tiles // step, block, (zero, zero, zero))


def field_defect(field, weights, out, s, where, amplitude, width):
    lane = lax.broadcasted_iota(jnp.int32, (8, LANES), 1)
    sub = lax.broadcasted_iota(jnp.int32, (8, LANES), 0)
    spot = where - (sub * width + lane)
    zero = jnp.zeros((8, LANES), F32)
    sums = [zero, zero]
    partial, east_at, west_at = None, None, zero

    def finish(j, to_left):
        done = partial - jnp.where(lane == LANES - 1, to_left, east_at)
        out[s, :, j * LANES : (j + 1) * LANES] = done
        sums[j % 2] = sums[j % 2] + done * done

    tiles = width // LANES
    for j in range(tiles):
        cols = slice(j * LANES, (j + 1) * LANES)
        h = field[s, 0:8, cols]
        halo = field[s, 8:16, cols]
        above = pltpu.roll(jnp.where(sub == 0, halo, h), 7, 0)
        below = pltpu.roll(jnp.where(sub == 7, halo, h), 1, 0)
        to_left = weights[4, :, cols] * h + weights[5, :, cols] * above
        to_right = weights[3, :, cols] * h + weights[6, :, cols] * below
        to_left = pltpu.roll(to_left, LANES - 1, 1)
        to_right = pltpu.roll(to_right, 1, 1)
        if j > 0:
            finish(j - 1, to_left)
        partial = (
            weights[0, :, cols] * h
            - weights[1, :, cols] * above
            - weights[2, :, cols] * below
            - jnp.where(lane == 0, west_at, to_right)
            - jnp.where(spot == j * LANES, amplitude, 0.0)
        )
        east_at, west_at = to_left, to_right
    finish(tiles - 1, zero)
    return sums[0] + sums[1]


def kernel(
    peers,
    amplitude,
    heat,
    cot_hbm,
    sources_hbm,
    out,
    norms,
    cot,
    sources,
    field,
    lower,
    weights,
    relay,
    row,
    rows,
    spare,
    stage,
    known,
    stage_sem,
    own_sem,
    cot_sem,
    src_sem,
    low_send,
    low_recv,
    part_recv,
    hand_recv,
    send,
    first_recv,
    near_recv,
    second_recv,
    edge_send,
    halo_send,
    halo_recv,
    relay_send,
    relay_recv,
    sum_send,
    sum_recv,
):
    v, k = lax.axis_index("vtx"), lax.axis_index("src")
    x = lax.rem(v, RING)
    per, _, width = field.shape
    groups, pieces = per // GROUP, per // PIECE
    tail = per - GROUP
    up, down = lax.rem(v + 1, peers), lax.rem(v + peers - 1, peers)
    line = v - x
    top, bottom = k == 3, k == 0
    last, first = x == RING - 1, x == 0

    around = [line + lax.rem(x + i, RING) for i in range(1, RING)]
    across = v + RING - 2 * RING * lax.rem(v // RING, 2)
    depth = [lax.rem(v + PLANE, peers), lax.rem(v + peers - PLANE, peers)]
    shared = [at(v, k ^ q) for q in (2, 3, 1)]
    around, across, depth = (
        [at(i, k) for i in around],
        [at(across, k)],
        [at(i, k) for i in depth],
    )

    barrier = pltpu.get_barrier_semaphore()
    near = shared + around + across + depth
    for target in near:
        signal(barrier, target)
    other = [2 - 2 * (k // 2) + core for core in (1, 0)]
    edge_row = jnp.where(top, 1, 0)
    staged = [
        pltpu.make_async_copy(
            heat.at[pl.ds(per * to, GROUP), edge_row], stage.at[i], stage_sem.at[i]
        )
        for i, to in enumerate(other)
    ]
    for copy in staged:
        copy.start()
    pl.semaphore_wait(barrier, len(near))

    def some(start, count):
        return pl.ds(start, count)

    def arrived(ref, sem):
        pltpu.make_async_copy(ref, ref, sem).wait()

    def exchange(to, r, start, count, sem):
        return remote(
            heat.at[pl.ds(per * to + start, count), r],
            field.at[some(start, count), 2 * k + r],
            send,
            sem,
            at(v, to),
        )

    def begin(g):
        for to in other:
            exchange(to, edge_row, g * GROUP, GROUP, first_recv.at[g]).start()

    for i, to in enumerate(other):
        staged[i].wait()
        remote(
            stage.at[i],
            field.at[0:GROUP, 2 * k + edge_row],
            send,
            first_recv.at[0],
            at(v, to),
        ).start()

    cot_copy = pltpu.make_async_copy(cot_hbm, cot, cot_sem)
    cot_copy.start()
    src_copy = pltpu.make_async_copy(sources_hbm, sources, src_sem)
    src_copy.start()
    own = pltpu.make_async_copy(
        heat.at[pl.ds(per * k, per)],
        field.at[:, pl.ds(pl.multiple_of(2 * k, 2), 2)],
        own_sem,
    )
    own.start()

    above_side = last & (k >= 2)
    below_side = first & (k < 2)
    holds = top | bottom
    own_row = jnp.where(top, 1, 0)
    block_row = jnp.where(k >= 2, 7, 0)
    split = (above_side | below_side) & holds
    helps = (above_side | below_side) & jnp.logical_not(holds)
    handed = remote(
        heat.at[pl.ds(per * (k ^ 3), per), own_row],
        spare,
        edge_send,
        hand_recv,
        at(v, k ^ 1),
    )

    @pl.when(split)
    def _():
        handed.start()

    def begin_near(g):
        remote(
            heat.at[pl.ds(per * (k ^ 1) + g * GROUP, GROUP)],
            field.at[some(g * GROUP, GROUP), pl.ds(pl.multiple_of(2 * k, 2), 2)],
            send,
            near_recv,
            at(v, k ^ 1),
        ).start()

    each(groups, begin_near)

    def meet(stage, targets):
        for target in targets:
            signal(known.at[stage], target)
        pl.semaphore_wait(known.at[stage], len(targets))

    meet(0, around)
    meet(1, across)
    meet(2, shared)

    half = width // 2
    cut = pl.ds(pl.multiple_of(lax.rem(k, 2) * half, half), half)
    low = remote(
        cot_hbm.at[pl.ds(2, 2), 7, cut],
        lower.at[:, 0, cut],
        low_send,
        low_recv,
        at(up, k),
    )
    low.start()

    arrived(field.at[:, 0:2], near_recv)

    @pl.when(helps)
    def _():
        handed.wait_recv()

    def wrap_copies(c):
        via = lax.rem(c, RING)
        slot = c // RING
        span = some(c * PIECE, PIECE)
        sem = c * PIECE // GROUP

        def send_on(src, m):
            for side, active, end, hop in (
                (0, above_side, 0, up),
                (1, below_side, RING - 1, down - (RING - 1)),
            ):

                @pl.when(active & (via == end))
                def _():
                    remote(
                        src,
                        field.at[span, (BELOW, ABOVE)[side]],
                        edge_send,
                        halo_recv.at[sem],
                        at(hop + via, m),
                    ).start()

                @pl.when(active & (via != end))
                def _():
                    remote(
                        src,
                        relay.at[side, slot],
                        edge_send,
                        relay_recv.at[side, slot],
                        at(hop + via, m),
                    ).start()

        @pl.when(split)
        def _():
            for m in (k, k ^ 2):
                send_on(heat.at[pl.ds(per * m + c * PIECE, PIECE), own_row], m)

        @pl.when(helps)
        def _():
            send_on(field.at[span, block_row], k)
            send_on(spare.at[span], k ^ 2)

    each(pieces, wrap_copies)

    def edge_copies(g):
        span = some(g * GROUP, GROUP)
        for i in range(2):

            @pl.when(top & jnp.logical_not(last))
            def _():
                m = 2 + i
                remote(
                    heat.at[pl.ds(per * m + g * GROUP, GROUP), 1],
                    field.at[span, BELOW],
                    edge_send,
                    halo_recv.at[g],
                    at(up, m),
                ).start()

            @pl.when(bottom & jnp.logical_not(first))
            def _():
                remote(
                    heat.at[pl.ds(per * i + g * GROUP, GROUP), 0],
                    field.at[span, ABOVE],
                    edge_send,
                    halo_recv.at[g],
                    at(down, i),
                ).start()

    each(groups, edge_copies)

    lax.fori_loop(1, groups, lambda g, _: (begin(g), 0)[1], 0)

    def begin_second(g):
        for to in other:
            exchange(to, 1 - edge_row, g * GROUP, GROUP, second_recv.at[g]).start()

    each(groups - 1, begin_second)

    def begin_last(n, to):
        exchange(to, 1 - edge_row, tail + n, 1, second_recv.at[groups - 1 + n]).start()

    for n in range(GROUP - 2):
        for to in other:
            begin_last(n, to)
    for to in other:
        for n in range(GROUP - 2, GROUP):
            begin_last(n, to)

    arrived(lower.at[:, 0, cut], low_recv)
    part = remote(
        lower.at[:, 0, cut], lower.at[:, 0, cut], low_send, part_recv, at(v, k ^ 1)
    )
    part.start()
    cot_copy.wait()
    src_copy.wait()
    part.wait_recv()
    shifted_weights(cot, lower, weights, v, peers * 8, width)
    meet(3, depth)

    inner_up = (k < 2) & jnp.logical_not(last)
    inner_down = (k >= 2) & jnp.logical_not(first)

    def forward(g):
        span = some(g * GROUP, GROUP)

        @pl.when(inner_up)
        def _():
            remote(
                field.at[span, 7],
                field.at[span, BELOW],
                halo_send,
                halo_recv.at[g],
                at(up, k),
            ).start()

        @pl.when(inner_down)
        def _():
            remote(
                field.at[span, 0],
                field.at[span, ABOVE],
                halo_send,
                halo_recv.at[g],
                at(down, k),
            ).start()

    relays_up = jnp.logical_not(first)
    relays_down = jnp.logical_not(last)

    def relayed(slot):
        c = x + RING * slot
        span = some(c * PIECE, PIECE)
        sem = c * PIECE // GROUP

        @pl.when(relays_up)
        def _():
            arrived(relay.at[0, slot], relay_recv.at[0, slot])
            remote(
                relay.at[0, slot],
                field.at[span, BELOW],
                relay_send.at[0],
                halo_recv.at[sem],
                at(line, k),
            ).start()

        @pl.when(relays_down)
        def _():
            arrived(relay.at[1, slot], relay_recv.at[1, slot])
            remote(
                relay.at[1, slot],
                field.at[span, ABOVE],
                relay_send.at[1],
                halo_recv.at[sem],
                at(line + RING - 1, k),
            ).start()

    for g in range(groups):
        if g == groups - 1:
            relayed(0)
        arrived(field.at[some(g * GROUP, GROUP), 0:2], first_recv.at[g])
        forward(g)
        if g % 2 == 1:
            meet(4 + g // 2, depth)

    own.wait()
    lane = lax.broadcasted_iota(jnp.int32, (1, LANES), 1)
    base = v * (8 * width)

    def group(g, sums):
        span = some(g * GROUP, GROUP)

        @pl.when(g == 1)
        def _():
            relayed(1)

        arrived(field.at[span, 0:2], halo_recv.at[g])
        only = g < groups - 1

        @pl.when(only)
        def _():
            arrived(field.at[span, 0:2], second_recv.at[g])

        def one(s, sums):
            @pl.when(jnp.logical_not(only))
            def _():
                arrived(field.at[pl.ds(s, 1), 0:2], second_recv.at[groups - 1 + s - tail])

            acc = field_defect(
                field,
                weights,
                out,
                s,
                sources[per * k + s] - base,
                amplitude,
                width,
            )
            total = jnp.sum(acc, axis=(0, 1), keepdims=True)
            return sums + jnp.where(lane == s, total, 0.0)

        return lax.fori_loop(g * GROUP, (g + 1) * GROUP, one, sums)

    sums = lax.fori_loop(0, groups, group, jnp.zeros((1, LANES), F32))

    row[...] = sums
    rows[0:1] = sums

    def tell(n, _):
        far = peers // 2 + PLANE - 1
        for step in range(TELL):
            i_step = 1 + lax.rem(far + peers - 2 - TELL * n - step, peers - 1)
            remote(
                row, rows.at[pl.ds(i_step, 1)], sum_send, sum_recv, at(lax.rem(v + i_step, peers), k)
            ).start()
        return 0

    lax.fori_loop(0, (peers - 1) // TELL, tell, 0)

    arrived(lower.at[:, 0], low_send)
    arrived(field.at[0 : 3 * per // 4, 0:8], send)

    inner = (top & jnp.logical_not(last)) | (bottom & jnp.logical_not(first))

    @pl.when(split)
    def _():
        arrived(field.at[:, 0:3], edge_send)

    @pl.when(helps | inner)
    def _():
        arrived(field.at[:, 0:2], edge_send)

    @pl.when(inner_up | inner_down)
    def _():
        arrived(field.at[:, 0:1], halo_send)

    @pl.when(relays_up)
    def _():
        arrived(relay.at[0], relay_send.at[0])

    @pl.when(relays_down)
    def _():
        arrived(relay.at[1], relay_send.at[1])

    arrived(rows.at[1:peers], sum_recv)
    sums = jnp.sum(rows[...], axis=0, keepdims=True)
    norms[...] = jnp.sqrt(sums / (peers * 8 * width) + 1e-06)
    arrived(rows.at[1:peers], sum_send)


def scale(defect, norms, out, held, sem):
    per = defect.shape[0]
    lane = lax.broadcasted_iota(jnp.int32, (per, per), 1)
    which = lax.broadcasted_iota(jnp.int32, (per, per), 0)
    own = jnp.where(lane == which, norms[...][None, :], 0.0)
    inverse = 1.0 / jnp.sum(own, axis=1, keepdims=True)
    copies, begun = [], 0
    for s in range(per):
        held[s] = defect[s] * inverse[s : s + 1]
        if s in STOPS:
            span = pl.ds(begun, s + 1 - begun)
            copies.append(
                pltpu.make_async_copy(held.at[span], out.at[span], sem.at[len(copies)])
            )
            copies[-1].start()
            begun = s + 1
    for copy in copies:
        copy.wait()


def on_device(heat, cotan, source_index):
    peers = lax.axis_size("vtx")
    rows_dev, width = cotan.shape[1:]
    per = heat.shape[0] // lax.axis_size("src")
    groups, slots = per // GROUP, per // PIECE // RING
    amplitude = math.sqrt(rows_dev * peers * width) / 8.0
    dma, vmem = pltpu.SemaphoreType.DMA, pltpu.VMEM
    anywhere = pl.BlockSpec(memory_space=pl.ANY)
    held = pl.BlockSpec(memory_space=pltpu.VMEM)
    block = jax.ShapeDtypeStruct((per, rows_dev, width), F32)
    defect, norms = pl.pallas_call(
        functools.partial(kernel, peers, amplitude),
        name="defect",
        out_shape=(block, jax.ShapeDtypeStruct((1, LANES), F32)),
        in_specs=[anywhere] * 3,
        out_specs=(held, held),
        scratch_shapes=[
            vmem((4, rows_dev, width), F32),
            pltpu.SMEM(source_index.shape, jnp.int32),
            vmem((per, 2 * rows_dev, width), F32),
            vmem((2, 8, width), F32),
            vmem((7, rows_dev, width), F32),
            vmem((2, slots, PIECE, width), F32),
            vmem((1, LANES), F32),
            vmem((peers, LANES), F32),
            vmem((per, width), F32),
            vmem((2, GROUP, width), F32),
            pltpu.SemaphoreType.REGULAR((6,)),
            dma((2,)),
            *[dma] * 8,
            dma((groups,)),
            dma,
            dma((groups - 1 + GROUP,)),
            dma,
            dma,
            dma((groups,)),
            dma((2,)),
            dma((2, slots)),
            dma,
            dma,
        ],
        compiler_params=pltpu.CompilerParams(
            collective_id=0, has_side_effects=True, vmem_limit_bytes=40 << 20
        ),
        cost_estimate=pl.CostEstimate(
            flops=200_000_000, bytes_accessed=16_000_000, transcendentals=0
        ),
    )(
        *(
            pltpu.with_memory_space_constraint(a, pltpu.HBM)
            for a in (heat, cotan, source_index)
        )
    )
    norms = norms[0, :per]
    normalised = pl.pallas_call(
        scale,
        name="scale",
        out_shape=block,
        in_specs=[held, held],
        out_specs=anywhere,
        scratch_shapes=[vmem(block.shape, F32), dma((len(STOPS),))],
        compiler_params=pltpu.CompilerParams(vmem_limit_bytes=16 << 20),
        cost_estimate=pl.CostEstimate(
            flops=4_000_000, bytes_accessed=8_400_000, transcendentals=0
        ),
    )(defect, norms)
    return (normalised, norms)


def solution(mesh):
    return jax.shard_map(
        on_device,
        mesh=mesh,
        in_specs=(P(None, ("vtx", "src"), None), P(None, "vtx", None), P()),
        out_specs=(P("src", "vtx", None), P("src")),
        check_vma=False,
    )
```
